128 devices in a mesh: node: 16 (over y, x), harm: 8 (over z, core).
Axes of the slice: x: 4, y: 4, z: 4, core: 2. Of those that a mesh axis runs over, the one named last changes fastest.
Arguments:
- krylov_basis: float32 [8, 2, 64, 32768], P(None, None, 'harm', 'node'), may hold values from -100 to 100, as said below
- cond_time: float32 [64, 32768], P('harm', 'node'), may hold values from 2 to 6
- capacity: float32 [32768], P('node'), may hold values from 0.005 to 0.05
- diag_blocks: float32 [128, 256, 256], P('node'), may hold values from -1 to 1
- coupling: float32 [128, 2, 256, 256], P('node'), may hold values from -0.375 to 0.375
- neighbours: int32 [128, 2], P('node'), may hold values from 0 to 127, as said below
- pattern: int32 [128, 2], P('node'), may hold values from 0 to 1
Outputs:
- new_vector: float32 [2, 64, 32768], P(None, 'harm', 'node')
- projections: float32 [2, 8], replicated
- new_norm: float32 [], replicated
The draws below stay inside these ranges and needn't reach their ends.
Inputs may be any that keep to these rules, and one draw needn't show every extreme that they name: `neighbours`: with the blocks in groups of 8 consecutive ones, each entry lies in a group 1 to 3 groups away from its row's group; the present slots of the rows of one group name at most 2 distinct blocks of any other group. `krylov_basis`: each of the 8 vectors has mean squared entry 1 over its real and imaginary parts.
All inputs are finite; a program needn't handle non-finite values.
Results may differ from the reference program's by a relative error of at most 0.0003.
Values sent between devices are 32-bit elements; how exact they have to be, the bound alone decides.
No kernel may reach another device: no remote copies, remote signals or barrier semaphores. Data moves between devices by JAX's collectives and lax.ppermute only.
A program may use at most 64 MiB of HBM per device.

```python
import math
import jax
import jax.numpy as jnp
from jax import lax

BS = 256
H = 64
BLK_DEV = 8
NEIGH = 2
KRY = 8
NS_ITERS = 4
USED = 2
BLOCKS = 128
NODES = 32768


def draw_krylov_basis(key, part):
    keys = jax.random.split(jax.random.fold_in(key, 11), 4)
    fresh = jax.random.truncated_normal(keys[0], -4.0, 4.0, (KRY, 2, H, BLOCKS * BS), jnp.float32)
    common = jax.random.truncated_normal(keys[1], -4.0, 4.0, (1, 2, H, BLOCKS * BS), jnp.float32)
    harmonic_scale = jnp.exp(jax.random.uniform(keys[2], (H,), jnp.float32, 0.0, math.log(10.0)))
    block_scale = jnp.exp(jax.random.uniform(keys[3], (BLOCKS,), jnp.float32, 0.0, math.log(10.0)))
    field = harmonic_scale[:, None] * jnp.repeat(block_scale, BS)[None, :]
    mixed = 0.85 * fresh + 0.5 * common
    vectors = field[None, None] * mixed
    spread = jnp.sqrt(jnp.mean(vectors * vectors, axis=(1, 2, 3), keepdims=True))
    return (vectors / spread).astype(jnp.float32)


def coupling_layout(key):
    keys = jax.random.split(jax.random.fold_in(key, 23), 5)
    groups = BLOCKS // BLK_DEV
    slots = BLK_DEV * NEIGH
    hot_keys = jax.random.split(keys[0], groups * 6)
    hot = jax.vmap(lambda k: jax.random.permutation(k, BLK_DEV))(hot_keys)[:, :USED]
    hot = hot.reshape(groups, 6, USED).astype(jnp.int32)
    slot_ids = jnp.arange(slots, dtype=jnp.int32)
    forced = jnp.broadcast_to(slot_ids < 6 * USED, (groups, slots))
    random_side = jax.random.randint(keys[1], (groups, slots), 0, 6, dtype=jnp.int32)
    random_pick = jax.random.randint(keys[2], (groups, slots), 0, USED, dtype=jnp.int32)
    side = jnp.where(forced, (slot_ids // USED)[None, :], random_side)
    pick = jnp.where(forced, (slot_ids % USED)[None, :], random_pick)
    order = jax.vmap(lambda k: jax.random.permutation(k, slots))(jax.random.split(keys[3], groups)).astype(jnp.int32)
    side = jnp.take_along_axis(side, order, axis=1)
    pick = jnp.take_along_axis(pick, order, axis=1)
    forced = jnp.take_along_axis(forced, order, axis=1)
    table = jnp.array([1, 2, 3, -1, -2, -3], dtype=jnp.int32)
    offsets = table[side]
    group = jnp.arange(groups, dtype=jnp.int32)[:, None]
    target = group + offsets
    flip = (target < 0) | (target >= groups)
    side = jnp.where(flip, (side + 3) % 6, side)
    target = jnp.where(flip, group - offsets, target)
    chosen = hot[group, side, pick]
    neighbours = (target * BLK_DEV + chosen).reshape(BLOCKS, NEIGH).astype(jnp.int32)
    present = (jax.random.randint(keys[4], (groups, slots), 0, 4, dtype=jnp.int32) > 0) | forced
    pattern = present.astype(jnp.int32).reshape(BLOCKS, NEIGH)
    return (neighbours, pattern)


def draw_neighbours(key, part):
    return coupling_layout(key)[0]


def draw_pattern(key, part):
    return coupling_layout(key)[1]


def level_of(own_key, extent, cuts, least, high):
    loudness = 1.0
    for axis_at, parts in cuts:
        draws = jax.random.uniform(jax.random.fold_in(jax.random.fold_in(own_key, 6), axis_at), (parts,), jnp.float32, least / len(cuts), high / len(cuts))
        loudness = loudness * jnp.repeat(jnp.exp(draws), extent[axis_at] // parts).reshape((-1,) + (1,) * (len(extent) - 1 - axis_at))
    return loudness


def scatter_about(rng, extent, scale, limit, shards=(), kind=jnp.bfloat16):
    drawn = jax.random.normal(rng, extent, jnp.float32) * scale
    if len(shards) > 0:
        drawn = level_of(rng, extent, shards, -0.22, 0.18) * drawn
    return jnp.clip(drawn, min=-limit, max=limit).astype(kind)


def setup_inputs(seed: int = 0) -> dict:
    key_list = jax.random.split(jax.random.key(seed), 8)
    return {
        "krylov_basis": draw_krylov_basis(jax.random.fold_in(key_list[7], 71), 0),
        "cond_time": jnp.clip(jnp.exp(math.log(6.0) - 1.0986123 * jax.random.uniform(key_list[1], (H, NODES), jnp.float32) ** level_of(key_list[1], (H, NODES), ((0, 8), (1, 16)), -0.2, 0.2)), 2.0, 6.0),
        "capacity": jnp.clip(jnp.exp(math.log(0.05) - 2.3025851 * jax.random.uniform(key_list[2], (NODES,), jnp.float32) ** level_of(key_list[2], (NODES,), ((0, 16),), -0.2, 0.2)), 0.005, 0.05),
        "diag_blocks": scatter_about(key_list[3], (BLOCKS, BS, BS), (BS // 8 + 2) ** -0.5, 1.0, ((0, 16),), jnp.float32),
        "coupling": scatter_about(key_list[4], (BLOCKS, NEIGH, BS, BS), BS ** -0.5, 0.375, ((0, 16),), jnp.float32),
        "neighbours": draw_neighbours(jax.random.fold_in(key_list[7], 71), 0),
        "pattern": draw_pattern(jax.random.fold_in(key_list[7], 71), 0),
    }


precise = lax.Precision.HIGHEST

def spectral_table(count):
    steps = jnp.arange(count, dtype=jnp.int32)
    phases = steps[:, None] * steps[None, :] % count
    angles = phases.astype(jnp.float32) * (2.0 * math.pi / count)
    factor = 1.0 / math.sqrt(count)
    cosine = jnp.cos(angles) * factor
    sine = jnp.sin(angles) * factor
    upper = jnp.concatenate([cosine, -sine], axis=1)
    lower = jnp.concatenate([sine, cosine], axis=1)
    return jnp.concatenate([upper, lower], axis=0)

def newton_inverse(blocks, means):
    width = blocks.shape[-1]
    identity = jnp.eye(width, dtype=jnp.float32)
    matrix = blocks + identity * means[:, None, :]
    inverse = identity * (1.0 / means)[:, None, :]
    for iteration in range(NS_ITERS):
        product = jnp.einsum('bij,bjk->bik', matrix, inverse, precision=precise)
        inverse = jnp.einsum('bij,bjk->bik', inverse, 2.0 * identity - product, precision=precise)
    return inverse

def reference(krylov_basis, cond_time, capacity, diag_blocks, coupling, neighbours, pattern):
    means = lax.optimization_barrier(jnp.sum(cond_time, axis=0)) / H
    inverse = newton_inverse(diag_blocks, means.reshape(BLOCKS, BS))
    vector = krylov_basis[KRY - 1].reshape(2, H, BLOCKS, BS)
    solved = jnp.einsum('bmn,phbn->phbm', inverse, vector, precision=precise)
    picked = jnp.take(solved, neighbours.reshape(-1).astype(jnp.int32), axis=2)
    picked = picked.reshape(2, H, BLOCKS, NEIGH, BS) * pattern.astype(jnp.float32)[None, None, :, :, None]
    coupled = jnp.einsum('bjmn,phbjn->phbm', coupling, picked, precision=precise).reshape(2, H, NODES)
    direct = jnp.einsum('bmn,phbn->phbm', diag_blocks, solved, precision=precise).reshape(2, H, NODES)
    table = spectral_table(H)
    samples = jnp.dot(table, solved.reshape(2 * H, NODES), precision=precise).reshape(2, H, NODES)
    driven = (samples * cond_time[None]).reshape(2 * H, NODES)
    spectra = jnp.dot(table.T, driven, precision=precise).reshape(2, H, NODES)
    solved_flat = solved.reshape(2, H, NODES)
    harmonics = jnp.arange(H, dtype=jnp.int32)
    omega = ((harmonics + H // 2) % H - H // 2).astype(jnp.float32)
    react = omega[:, None] * capacity[None, :]
    image_real = direct[0] + spectra[0] + coupled[0] - react * solved_flat[1]
    image_imag = direct[1] + spectra[1] + coupled[1] + react * solved_flat[0]
    count = H * NODES
    basis_real = krylov_basis[:, 0].reshape(KRY, -1)
    basis_imag = krylov_basis[:, 1].reshape(KRY, -1)
    flat_real = image_real.reshape(-1)
    flat_imag = image_imag.reshape(-1)
    proj_real = (jnp.dot(basis_real, flat_real, precision=precise) + jnp.dot(basis_imag, flat_imag, precision=precise)) / count
    proj_imag = (jnp.dot(basis_real, flat_imag, precision=precise) - jnp.dot(basis_imag, flat_real, precision=precise)) / count
    rest_real = flat_real - (jnp.dot(proj_real, basis_real, precision=precise) - jnp.dot(proj_imag, basis_imag, precision=precise))
    rest_imag = flat_imag - (jnp.dot(proj_real, basis_imag, precision=precise) + jnp.dot(proj_imag, basis_real, precision=precise))
    squares = (jnp.sum(rest_real * rest_real) + jnp.sum(rest_imag * rest_imag)) / count
    new_norm = jnp.sqrt(squares + 1e-06)
    new_vector = jnp.stack([rest_real, rest_imag]).reshape(2, H, NODES) / new_norm
    return (new_vector, jnp.stack([proj_real, proj_imag]), new_norm)
```

```python
import math

import jax
import jax.numpy as jnp
import numpy as np
from jax import lax
from jax.experimental import pallas as pl
from jax.experimental.pallas import tpu as pltpu
from jax.sharding import Mesh
from jax.sharding import PartitionSpec as P

BS = 256
H = 64
NEIGH = 2
KRY = 8
HARM = ("harm_0", "harm_1")
NODE = ("node_0", "node_1")
NODE_HARM = ("node_0", "node_1", "harm_0", "harm_1")
F32 = jnp.float32
BF16 = jnp.bfloat16
LANES = 128
GRAM = 64
SMEM = pl.BlockSpec(memory_space=pltpu.SMEM)
VMEM = pl.BlockSpec(memory_space=pltpu.VMEM)


def spectral_tables():
    steps = np.arange(H)
    angles = (steps[:, None] * steps[None, :] % H) * (2.0 * math.pi / H)
    cosine = np.cos(angles) / math.sqrt(H)
    sine = np.sin(angles) / math.sqrt(H)
    table = np.block([[cosine, -sine], [sine, cosine]]).astype(np.float32)
    both = np.stack([table, table.T])
    high = both.astype(jnp.bfloat16)
    low = (both - high.astype(np.float32)).astype(jnp.bfloat16)
    return high, low


def split(x):
    high = x.astype(BF16)
    return high, (x - high.astype(F32)).astype(BF16)


def mm(a, b):
    return jnp.dot(a, b, preferred_element_type=F32)


def mm_t(a, b):
    return lax.dot_general(a, b, (((1,), (1,)), ((), ())), preferred_element_type=F32)


def rows_mm(x, w_high, w_low, product=mm):
    rows = x.shape[0]
    high, low = split(x)
    both = product(jnp.concatenate([high, low], axis=0), w_high)
    return both[:rows] + both[rows:] + product(high, w_low)


def sublane_sum(x):
    return jnp.sum(x, axis=0, keepdims=True)


def rows_to_lanes(rows):
    return sublane_sum(jnp.transpose(rows))


def pack_kernel(nb_ref, pat_ref, v_ref, cond_ref, out_ref, hot_ref):
    blk = out_ref.shape[0]
    sums = jnp.concatenate(
        [sublane_sum(cond_ref[:, BS * b : BS * (b + 1)]) for b in range(blk)], axis=0
    )
    for b in range(blk):
        cols = slice(BS * b, BS * (b + 1))
        out_ref[b, 0] = v_ref[0, 0, :, cols]
        out_ref[b, 1] = v_ref[0, 1, :, cols]
        out_ref[b, 2] = cond_ref[:, cols]
        out_ref[b, 3] = sums
    groups = hot_ref.shape[0]
    for q in range(groups):
        hot_ref[q, 0] = blk
        hot_ref[q, 1] = -1
    for b in range(blk):
        for j in range(NEIGH):
            block = nb_ref[b, j]
            group = block // blk
            local = block - group * blk

            @pl.when(pat_ref[b, j] > 0)
            def _():
                hot_ref[group, 0] = jnp.minimum(hot_ref[group, 0], local)
                hot_ref[group, 1] = jnp.maximum(hot_ref[group, 1], local)


def prep_kernel(diag_ref, k_ref, t_ref, gram_ref, rows):
    for b in range(diag_ref.shape[0]):
        t_ref[b] = jnp.transpose(diag_ref[b])
    rows[...] = jnp.zeros_like(rows)
    chunks = k_ref.shape[3] // LANES
    for m in range(KRY):
        real = [None] * KRY
        imag = [None] * KRY
        for c in range(chunks):
            cols = slice(LANES * c, LANES * (c + 1))
            mr, mi = k_ref[m, 0, :, cols], k_ref[m, 1, :, cols]
            for n in range(m, KRY):
                nr, ni = (mr, mi) if n == m else (k_ref[n, 0, :, cols], k_ref[n, 1, :, cols])
                r = mr * nr + mi * ni
                real[n] = r if c == 0 else real[n] + r
                if n > m:
                    i = mr * ni - mi * nr
                    imag[n] = i if c == 0 else imag[n] + i
        for n in range(m, KRY):
            at = GRAM + KRY * m + n
            rows[at : at + 1] = sublane_sum(real[n])
            if n > m:
                at = GRAM + KRY * n + m
                rows[at : at + 1] = sublane_sum(imag[n])
    gram_ref[...] = rows_to_lanes(rows[...])


def solve_kernel(place_ref, hot_ref, got_ref, t_ref, v_ref, send_ref, own_ref, means_ref, e_ref, row_ref, d_ref):
    blk = t_ref.shape[0]
    half = v_ref.shape[2]
    means = got_ref[0, 3]
    for s in range(1, got_ref.shape[0]):
        means = means + got_ref[s, 3]
    means = means * (1.0 / H)
    means_ref[...] = means
    d_ref[...] = 1.0 / means

    def one(b):
        d = d_ref[pl.ds(b, 1), :]
        cols = pl.ds(pl.multiple_of(b * BS, BS), BS)
        power = t_ref[b] * (-d)
        u = jnp.concatenate([v_ref[0, 0, :, cols], v_ref[0, 1, :, cols]], axis=0) * d
        for p in range(4):
            high, low = split(power)
            e_ref[b, p, 0] = high
            e_ref[b, p, 1] = low
            u = u + rows_mm(u, high, low)
            if p < 3:
                both = mm(jnp.concatenate([high, low], axis=0), high)
                power = both[:BS] + both[BS:] + mm(high, low)
        row_ref[b, 0] = u[:half]
        row_ref[b, 1] = u[half:]

    def pair(i, carry):
        one(2 * i)
        one(2 * i + 1)
        return carry

    lax.fori_loop(0, blk // 2, pair, 0)

    me = place_ref[0]
    own = place_ref[1]
    own_ref[...] = e_ref[own]
    groups = send_ref.shape[0]
    for q in range(groups):
        send_ref[q] = jnp.zeros(send_ref.shape[1:], F32)
    for offset in (1, 2, 3, -1, -2, -3):
        group = me + offset

        @pl.when((group >= 0) & (group < groups))
        def _():
            first = jnp.minimum(hot_ref[group, 0], blk - 1)
            second = jnp.maximum(hot_ref[group, 1], 0)
            send_ref[group, 0:2] = row_ref[first]
            send_ref[group, 2:4] = row_ref[second]


def column_kernel(place_ref, got_ref, own_ref, means_ref, cap_ref, omega_ref, high_ref, low_ref, out_ref):
    sources = got_ref.shape[0]
    own = place_ref[1]
    mean = means_ref[pl.ds(own, 1), :]
    u = jnp.concatenate([got_ref[s, p] for p in range(2) for s in range(sources)], axis=0)
    u = u * (1.0 / mean)
    for p in range(4):
        u = u + rows_mm(u, own_ref[p, 0], own_ref[p, 1])
    direct = rows_mm(u, own_ref[0, 0], own_ref[0, 1]) * (-mean)

    def transform(way, x):
        high, low = split(x)
        table = high_ref[way]
        return mm(table, high) + mm(table, low) + mm(low_ref[way], high)

    cond = jnp.concatenate([got_ref[s, 2] for s in range(sources)], axis=0)
    driven = transform(0, u) * jnp.concatenate([cond, cond], axis=0)
    image = direct + transform(1, driven)
    react = omega_ref[...] * cap_ref[pl.ds(own, 1), :]
    real = image[:H] - react * u[H:]
    imag = image[H:] + react * u[:H]
    step = H // sources
    for s in range(sources):
        out_ref[s, 0] = real[step * s : step * (s + 1)]
        out_ref[s, 1] = imag[step * s : step * (s + 1)]


def image_kernel(nb_ref, pat_ref, hot_ref, back_ref, got_ref, c_ref, k_ref, gram_ref, image_ref, send_ref, rows):
    blk = c_ref.shape[0]
    half = k_ref.shape[2]

    def one(b):
        total = jnp.concatenate([back_ref[b, 0], back_ref[b, 1]], axis=0)
        for j in range(NEIGH):
            block = nb_ref[b, j]
            group = block // blk
            second = jnp.where(block - group * blk == hot_ref[group, 0], 0, 2)
            x = jnp.concatenate([got_ref[group, second], got_ref[group, second + 1]], axis=0)
            x = x * pat_ref[b, j].astype(F32)
            total = total + rows_mm(x, *split(c_ref[b, j]), product=mm_t)
        cols = pl.ds(pl.multiple_of(b * BS, BS), BS)
        image_ref[0, :, cols] = total[:half]
        image_ref[1, :, cols] = total[half:]

    def pair(i, carry):
        one(2 * i)
        one(2 * i + 1)
        return carry

    lax.fori_loop(0, blk // 2, pair, 0)

    chunks = k_ref.shape[3] // LANES
    real = [None] * KRY
    imag = [None] * KRY
    squares = None
    for c in range(chunks):
        cols = slice(LANES * c, LANES * (c + 1))
        ir, ii = image_ref[0, :, cols], image_ref[1, :, cols]
        both = ir * ir + ii * ii
        squares = both if c == 0 else squares + both
        for m in range(KRY):
            mr, mi = k_ref[m, 0, :, cols], k_ref[m, 1, :, cols]
            r = mr * ir + mi * ii
            i = mr * ii - mi * ir
            real[m] = r if c == 0 else real[m] + r
            imag[m] = i if c == 0 else imag[m] + i
    rows[...] = jnp.zeros_like(rows)
    for m in range(KRY):
        rows[m : m + 1] = sublane_sum(real[m])
        rows[KRY + m : KRY + m + 1] = sublane_sum(imag[m])
    rows[2 * KRY : 2 * KRY + 1] = sublane_sum(squares)
    row = rows_to_lanes(rows[...]) + gram_ref[...]
    send_ref[...] = jnp.broadcast_to(row, send_ref.shape)


def rest_kernel(count, got_ref, image_ref, k_ref, vector_ref, proj_ref, norm_ref):
    totals = sublane_sum(got_ref[...]) * (1.0 / count)
    lane = lax.broadcasted_iota(jnp.int32, totals.shape, 1)

    def at(q):
        return jnp.broadcast_to(totals[:, q : q + 1], totals.shape)

    pr = [at(m) for m in range(KRY)]
    pi = [at(KRY + m) for m in range(KRY)]
    row_r = row_i = col_r = col_i = jnp.zeros_like(totals)
    row_of = (lane - GRAM) // KRY
    col_of = (lane - GRAM) - row_of * KRY
    for m in range(KRY):
        row_r = jnp.where(row_of == m, pr[m], row_r)
        row_i = jnp.where(row_of == m, pi[m], row_i)
        col_r = jnp.where(col_of == m, pr[m], col_r)
        col_i = jnp.where(col_of == m, pi[m], col_i)
    upper = row_r * col_r + row_i * col_i
    lower = col_i * row_r - col_r * row_i
    weight = jnp.where(row_of == col_of, upper, 2.0 * jnp.where(row_of < col_of, upper, lower))
    weight = jnp.where(lane >= GRAM, weight, 0.0)
    weight = jnp.where(lane < 2 * KRY, -2.0 * totals, weight)
    weight = jnp.where(lane == 2 * KRY, 1.0, weight)
    squares = jnp.sum(totals * weight, axis=1, keepdims=True)
    norm = jnp.sqrt(squares + 1e-06)
    norm_ref[...] = norm
    for m in range(KRY):
        proj_ref[0:1, m : m + 1] = pr[m][:, 0:1]
        proj_ref[1:2, m : m + 1] = pi[m][:, 0:1]
    half = k_ref.shape[2]
    scale = jnp.broadcast_to(1.0 / norm, (half, LANES))
    pr = [jnp.broadcast_to(x, (half, LANES)) for x in pr]
    pi = [jnp.broadcast_to(x, (half, LANES)) for x in pi]
    for c in range(k_ref.shape[3] // LANES):
        cols = slice(LANES * c, LANES * (c + 1))
        real, imag = image_ref[0, :, cols], image_ref[1, :, cols]
        for m in range(KRY):
            mr, mi = k_ref[m, 0, :, cols], k_ref[m, 1, :, cols]
            real = real - (pr[m] * mr - pi[m] * mi)
            imag = imag - (pr[m] * mi + pi[m] * mr)
        vector_ref[0, :, cols] = real * scale
        vector_ref[1, :, cols] = imag * scale


def struct(*dims, dtype=F32):
    return jax.ShapeDtypeStruct(dims, dtype)


def call(kernel, out_shape, in_specs, out_specs, name, flops, scratch=(), **kw):
    return pl.pallas_call(
        kernel,
        out_shape=out_shape,
        in_specs=in_specs,
        out_specs=out_specs,
        scratch_shapes=list(scratch),
        name=name,
        cost_estimate=pl.CostEstimate(flops=flops, bytes_accessed=1 << 20, transcendentals=0),
        **kw,
    )


def exchange(x, axes):
    return lax.all_to_all(x, axes, split_axis=0, concat_axis=0, tiled=True)


def per_device(krylov_basis, cond_time, capacity, diag_blocks, coupling, neighbours, pattern):
    h_dev = krylov_basis.shape[2]
    nodes_dev = krylov_basis.shape[3]
    blk = diag_blocks.shape[0]
    harm = lax.axis_size(HARM)
    groups = lax.axis_size(NODE)
    world = groups * harm
    place = jnp.stack([lax.axis_index(NODE), lax.axis_index(HARM)]).astype(jnp.int32)
    last = pl.BlockSpec((1, 2, h_dev, nodes_dev), lambda i: (KRY - 1, 0, 0, 0))

    packed, hot_own = call(
        pack_kernel,
        (struct(blk, 4, h_dev, BS), struct(groups, LANES, dtype=jnp.int32)),
        [SMEM, SMEM, last, pl.BlockSpec((h_dev, nodes_dev), lambda i: (0, 0))],
        (pl.BlockSpec((blk, 4, h_dev, BS), lambda i: (0, 0, 0, 0)), SMEM),
        "pack",
        1 << 20,
        grid=(1,),
    )(neighbours, pattern, krylov_basis, cond_time)
    got = exchange(packed, HARM)
    hot = exchange(hot_own, NODE)
    turned, gram = call(
        prep_kernel,
        (struct(blk, BS, BS), struct(1, LANES)),
        [VMEM, VMEM],
        (VMEM, VMEM),
        "prep",
        1 << 28,
        [pltpu.VMEM((LANES, LANES), F32)],
    )(diag_blocks, krylov_basis)
    whole = lambda *dims: pl.BlockSpec(dims, lambda i: (0,) * len(dims))
    send_hot, own, means = call(
        solve_kernel,
        (struct(groups, 4, h_dev, BS), struct(4, 2, BS, BS, dtype=BF16), struct(blk, BS)),
        [SMEM, SMEM, whole(harm, 4, h_dev, BS), whole(blk, BS, BS), last],
        (whole(groups, 4, h_dev, BS), whole(4, 2, BS, BS), whole(blk, BS)),
        "solve",
        1 << 31,
        [
            pltpu.VMEM((blk, 4, 2, BS, BS), BF16),
            pltpu.VMEM((blk, 2, h_dev, BS), F32),
            pltpu.VMEM((blk, BS), F32),
        ],
        grid=(1,),
    )(place, hot, got, turned, krylov_basis)
    named = exchange(send_hot, NODE)
    high, low = spectral_tables()
    omega = np.broadcast_to((((np.arange(H) + H // 2) % H) - H // 2).astype(np.float32)[:, None], (H, BS))
    send_cols = call(
        column_kernel,
        struct(harm, 2, h_dev, BS),
        [SMEM] + [VMEM] * 7,
        VMEM,
        "column",
        1 << 27,
    )(place, got, own, means, capacity.reshape(blk, BS), jnp.asarray(omega), jnp.asarray(high), jnp.asarray(low))
    back = exchange(send_cols, HARM)
    image, send_sums = call(
        image_kernel,
        (struct(2, h_dev, nodes_dev), struct(world, LANES)),
        [SMEM] * 3 + [VMEM] * 5,
        (VMEM, VMEM),
        "image",
        1 << 28,
        [pltpu.VMEM((LANES, LANES), F32)],
    )(neighbours, pattern, hot_own, back, named, coupling, krylov_basis, gram)
    sums = exchange(send_sums, NODE_HARM)
    count = world * h_dev * nodes_dev
    vector, proj, norm = call(
        lambda *refs: rest_kernel(count, *refs),
        (struct(2, h_dev, nodes_dev), struct(2, KRY), struct(1, 1)),
        [VMEM] * 3,
        (VMEM, VMEM, VMEM),
        "rest",
        1 << 24,
    )(sums, image, krylov_basis)
    return vector, proj, norm.reshape(())


def solution(mesh):
    finer = Mesh(mesh.devices.reshape(4, 4, 4, 2), ("node_0", "node_1", "harm_0", "harm_1"))
    placed = (
        P(None, None, HARM, NODE),
        P(HARM, NODE),
        P(NODE),
        P(NODE, None, None),
        P(NODE, None, None, None),
        P(NODE, None),
        P(NODE, None),
    )
    return jax.shard_map(
        per_device,
        mesh=finer,
        in_specs=placed,
        out_specs=(P(None, HARM, NODE), P(), P()),
        check_vma=False,
    )
```

```python
import math

import jax
import jax.numpy as jnp
import numpy as np
from jax import lax
from jax.experimental import pallas as pl
from jax.experimental.pallas import tpu as pltpu
from jax.sharding import Mesh
from jax.sharding import PartitionSpec as P

BS = 256
H = 64
NEIGH = 2
KRY = 8
HARM = ("harm_0", "harm_1")
NODE = ("node_0", "node_1")
NODE_HARM = ("node_0", "node_1", "harm_0", "harm_1")
F32 = jnp.float32
BF16 = jnp.bfloat16
LANES = 128
GRAM = 64
SMEM = pl.BlockSpec(memory_space=pltpu.SMEM)
VMEM = pl.BlockSpec(memory_space=pltpu.VMEM)
ANY = pl.BlockSpec(memory_space=pl.ANY)


def spectral_tables():
    steps = np.arange(H)
    angles = (steps[:, None] * steps[None, :] % H) * (2.0 * math.pi / H)
    cosine = np.cos(angles) / math.sqrt(H)
    sine = np.sin(angles) / math.sqrt(H)
    table = np.block([[cosine, -sine], [sine, cosine]]).astype(np.float32)
    both = np.stack([table, table.T])
    high = both.astype(jnp.bfloat16)
    low = (both - high.astype(np.float32)).astype(jnp.bfloat16)
    return high, low


def split(x):
    high = x.astype(BF16)
    return high, (x - high.astype(F32)).astype(BF16)


def mm(a, b):
    return jnp.dot(a, b, preferred_element_type=F32)


def mm_t(a, b):
    return lax.dot_general(a, b, (((1,), (1,)), ((), ())), preferred_element_type=F32)


def rows_mm(x, w_high, w_low, product=mm):
    rows = x.shape[0]
    high, low = split(x)
    both = product(jnp.concatenate([high, low], axis=0), w_high)
    return both[:rows] + both[rows:] + product(high, w_low)


def sublane_sum(x):
    return jnp.sum(x, axis=0, keepdims=True)


def rows_to_lanes(rows):
    return sublane_sum(jnp.transpose(rows))


def index_kernel(nb_ref, pat_ref, hot_ref):
    groups = hot_ref.shape[0]
    blk = nb_ref.shape[1]
    for q in range(groups):
        hot_ref[q, 0] = blk
        hot_ref[q, 1] = -1
    for b in range(blk):
        for j in range(NEIGH):
            block = nb_ref[j, b]
            group = block // blk
            local = block - group * blk

            @pl.when(pat_ref[j, b] > 0)
            def _():
                hot_ref[group, 0] = jnp.minimum(hot_ref[group, 0], local)
                hot_ref[group, 1] = jnp.maximum(hot_ref[group, 1], local)


def pack_kernel(k_ref, cond_ref, out_ref, held, sem):
    copy = pltpu.make_async_copy(k_ref.at[KRY - 1], held, sem)
    copy.start()
    blk = out_ref.shape[0]
    sums = jnp.concatenate(
        [sublane_sum(cond_ref[:, BS * b : BS * (b + 1)]) for b in range(blk)], axis=0
    )
    for b in range(blk):
        out_ref[b, 2] = cond_ref[:, BS * b : BS * (b + 1)]
        out_ref[b, 3] = sums
    copy.wait()
    for b in range(blk):
        cols = slice(BS * b, BS * (b + 1))
        out_ref[b, 0] = held[0, :, cols]
        out_ref[b, 1] = held[1, :, cols]


def turn_kernel(diag_ref, t_ref, held, sems):
    blk = t_ref.shape[0]
    copies = [pltpu.make_async_copy(diag_ref.at[b], held.at[b], sems.at[b]) for b in range(blk)]
    for copy in copies:
        copy.start()
    for b, copy in enumerate(copies):
        copy.wait()
        t_ref[b] = jnp.transpose(held[b])


def gram_kernel(k_ref, gram_ref, rows):
    rows[...] = jnp.zeros_like(rows)
    chunks = k_ref.shape[3] // LANES
    for m in range(KRY):
        real = [None] * KRY
        imag = [None] * KRY
        for c in range(chunks):
            cols = slice(LANES * c, LANES * (c + 1))
            mr, mi = k_ref[m, 0, :, cols], k_ref[m, 1, :, cols]
            for n in range(m, KRY):
                nr, ni = (mr, mi) if n == m else (k_ref[n, 0, :, cols], k_ref[n, 1, :, cols])
                r = mr * nr + mi * ni
                real[n] = r if c == 0 else real[n] + r
                if n > m:
                    i = mr * ni - mi * nr
                    imag[n] = i if c == 0 else imag[n] + i
        for n in range(m, KRY):
            at = GRAM + KRY * m + n
            rows[at : at + 1] = sublane_sum(real[n])
            if n > m:
                at = GRAM + KRY * n + m
                rows[at : at + 1] = sublane_sum(imag[n])
    gram_ref[...] = rows_to_lanes(rows[...])


def powers_of(e_ref, b, at, turned, d):
    e_ref[b, at, 0], e_ref[b, at, 1] = split(turned * (-d))


def squared_with(e_ref, u_ref, b, p):
    high, low = e_ref[b, p, 0], e_ref[b, p, 1]
    u = u_ref[b]
    rows = u.shape[0]
    u_high, u_low = split(u)
    x = mm(jnp.concatenate([high, low, u_high, u_low], axis=0), high)
    y = mm(jnp.concatenate([high, u_high], axis=0), low)
    u_ref[b] = u + (x[2 * BS : 2 * BS + rows] + x[2 * BS + rows :] + y[BS:])
    e_ref[b, p + 1, 0], e_ref[b, p + 1, 1] = split(x[:BS] + x[BS : 2 * BS] + y[:BS])


def solve_kernel(got_ref, t_ref, k_ref, means_ref, u_ref, e_ref, d_ref):
    blk = t_ref.shape[0]
    powers = e_ref.shape[1]
    means = got_ref[0, 3]
    for s in range(1, got_ref.shape[0]):
        means = means + got_ref[s, 3]
    means = means * (1.0 / H)
    means_ref[...] = means
    d_ref[...] = 1.0 / means
    for b in range(blk):
        d = d_ref[b : b + 1]
        powers_of(e_ref, b, 0, t_ref[b], d)
        cols = slice(b * BS, (b + 1) * BS)
        u_ref[b] = jnp.concatenate([k_ref[KRY - 1, 0, :, cols], k_ref[KRY - 1, 1, :, cols]], axis=0) * d

    def stage(p, carry):
        for b in range(blk):
            squared_with(e_ref, u_ref, b, p)
        return carry

    lax.fori_loop(0, powers - 1, stage, 0)
    for b in range(blk):
        u = u_ref[b]
        u_ref[b] = u + rows_mm(u, e_ref[b, powers - 1, 0], e_ref[b, powers - 1, 1])
    for b in range(blk):
        u = u_ref[b]
        twice = rows_mm(u, e_ref[b, powers - 1, 0], e_ref[b, powers - 1, 1])
        u_ref[b] = u + rows_mm(twice, e_ref[b, powers - 1, 0], e_ref[b, powers - 1, 1])


def select_kernel(hot_ref, u_ref, send_ref, sems):
    blk = u_ref.shape[0]
    groups = send_ref.shape[0]
    me = lax.axis_index(NODE)
    for wait in (False, True):
        for at, offset in enumerate((1, 2, 3, -1, -2, -3)):
            group = me + offset

            @pl.when((group >= 0) & (group < groups))
            def _():
                first = jnp.minimum(hot_ref[group, 0], blk - 1)
                second = jnp.maximum(hot_ref[group, 1], 0)
                for slot, b in enumerate((first, second)):
                    copy = pltpu.make_async_copy(u_ref.at[b], send_ref.at[group, slot], sems.at[at, slot])
                    if wait:
                        copy.wait()
                    else:
                        copy.start()


def column_kernel(got_ref, diag_ref, means_ref, cap_ref, high_ref, low_ref, out_ref, held, sem, u_ref, e_ref):
    own = lax.axis_index(HARM)
    copy = pltpu.make_async_copy(diag_ref.at[own], held, sem)
    copy.start()
    sources = got_ref.shape[0]
    powers = e_ref.shape[1]
    mean = means_ref[pl.ds(own, 1), :]
    d = 1.0 / mean
    u_ref[0] = jnp.concatenate([got_ref[s, p] for p in range(2) for s in range(sources)], axis=0) * d
    copy.wait()
    powers_of(e_ref, 0, 0, jnp.transpose(held[...]), d)
    for p in range(powers - 1):
        squared_with(e_ref, u_ref, 0, p)
    u = u_ref[0]
    u = u + rows_mm(u, e_ref[0, powers - 1, 0], e_ref[0, powers - 1, 1])
    twice = rows_mm(u, e_ref[0, powers - 1, 0], e_ref[0, powers - 1, 1])
    u = u + rows_mm(twice, e_ref[0, powers - 1, 0], e_ref[0, powers - 1, 1])
    direct = rows_mm(u, e_ref[0, 0, 0], e_ref[0, 0, 1]) * (-mean)

    def transform(way, x):
        high, low = split(x)
        table = high_ref[way]
        return mm(table, high) + mm(table, low) + mm(low_ref[way], high)

    cond = jnp.concatenate([got_ref[s, 2] for s in range(sources)], axis=0)
    driven = transform(0, u) * jnp.concatenate([cond, cond], axis=0)
    image = direct + transform(1, driven)
    cap = cap_ref[pl.ds(pl.multiple_of(own * BS, BS), BS)].reshape(1, BS)
    harmonic = lax.broadcasted_iota(jnp.int32, (H, BS), 0)
    omega = jnp.where(harmonic < H // 2, harmonic, harmonic - H)
    react = omega.astype(F32) * cap
    real = image[:H] - react * u[H:]
    imag = image[H:] + react * u[:H]
    step = H // sources
    for s in range(sources):
        out_ref[s, 0] = real[step * s : step * (s + 1)]
        out_ref[s, 1] = imag[step * s : step * (s + 1)]


def couple_kernel(nb_ref, pat_ref, hot_ref, got_ref, c_ref, out_ref, held, sems):
    blk = held.shape[0]
    half = out_ref.shape[1]
    copies = [pltpu.make_async_copy(c_ref.at[b], held.at[b], sems.at[b]) for b in range(blk)]
    for copy in copies:
        copy.start()
    for b, copy in enumerate(copies):
        copy.wait()
        total = None
        for j in range(NEIGH):
            block = nb_ref[j, b]
            group = block // blk
            second = jnp.where(block - group * blk == hot_ref[group, 0], 0, 1)
            x = jnp.where(pat_ref[j, b] > 0, got_ref[group, second], 0.0)
            term = rows_mm(x, *split(held[b, j]), product=mm_t)
            total = term if j == 0 else total + term
        cols = slice(b * BS, (b + 1) * BS)
        out_ref[0, :, cols] = total[:half]
        out_ref[1, :, cols] = total[half:]


def image_kernel(back_ref, coupled_ref, k_ref, gram_ref, image_ref, send_ref, rows):
    chunks = k_ref.shape[3] // LANES
    real = [None] * KRY
    imag = [None] * KRY
    squares = None
    for c in range(chunks):
        cols = slice(LANES * c, LANES * (c + 1))
        block, at = LANES * c // BS, LANES * c % BS
        ir = coupled_ref[0, :, cols] + back_ref[block, 0, :, at : at + LANES]
        ii = coupled_ref[1, :, cols] + back_ref[block, 1, :, at : at + LANES]
        image_ref[0, :, cols] = ir
        image_ref[1, :, cols] = ii
        both = ir * ir + ii * ii
        squares = both if c == 0 else squares + both
        for m in range(KRY):
            mr, mi = k_ref[m, 0, :, cols], k_ref[m, 1, :, cols]
            r = mr * ir + mi * ii
            i = mr * ii - mi * ir
            real[m] = r if c == 0 else real[m] + r
            imag[m] = i if c == 0 else imag[m] + i
    rows[...] = jnp.zeros_like(rows)
    for m in range(KRY):
        rows[m : m + 1] = sublane_sum(real[m])
        rows[KRY + m : KRY + m + 1] = sublane_sum(imag[m])
    rows[2 * KRY : 2 * KRY + 1] = sublane_sum(squares)
    row = rows_to_lanes(rows[...]) + gram_ref[...]
    send_ref[...] = jnp.broadcast_to(row, send_ref.shape)


def rest_kernel(count, got_ref, image_ref, k_ref, vector_ref, proj_ref, norm_ref):
    totals = sublane_sum(got_ref[...]) * (1.0 / count)
    lane = lax.broadcasted_iota(jnp.int32, totals.shape, 1)

    def at(q):
        return jnp.broadcast_to(totals[:, q : q + 1], totals.shape)

    pr = [at(m) for m in range(KRY)]
    pi = [at(KRY + m) for m in range(KRY)]
    row_r = row_i = col_r = col_i = jnp.zeros_like(totals)
    row_of = (lane - GRAM) // KRY
    col_of = (lane - GRAM) - row_of * KRY
    for m in range(KRY):
        row_r = jnp.where(row_of == m, pr[m], row_r)
        row_i = jnp.where(row_of == m, pi[m], row_i)
        col_r = jnp.where(col_of == m, pr[m], col_r)
        col_i = jnp.where(col_of == m, pi[m], col_i)
    upper = row_r * col_r + row_i * col_i
    lower = col_i * row_r - col_r * row_i
    weight = jnp.where(row_of == col_of, upper, 2.0 * jnp.where(row_of < col_of, upper, lower))
    weight = jnp.where(lane >= GRAM, weight, 0.0)
    weight = jnp.where(lane < 2 * KRY, -2.0 * totals, weight)
    weight = jnp.where(lane == 2 * KRY, 1.0, weight)
    squares = jnp.sum(totals * weight, axis=1, keepdims=True)
    norm = jnp.sqrt(squares + 1e-06)
    norm_ref[...] = norm
    for m in range(KRY):
        proj_ref[0:1, m : m + 1] = pr[m][:, 0:1]
        proj_ref[1:2, m : m + 1] = pi[m][:, 0:1]
    half = k_ref.shape[2]
    scale = jnp.broadcast_to(1.0 / norm, (half, LANES))
    pr = [jnp.broadcast_to(x, (half, LANES)) for x in pr]
    pi = [jnp.broadcast_to(x, (half, LANES)) for x in pi]
    for c in range(k_ref.shape[3] // LANES):
        cols = slice(LANES * c, LANES * (c + 1))
        real, imag = image_ref[0, :, cols], image_ref[1, :, cols]
        for m in range(KRY):
            mr, mi = k_ref[m, 0, :, cols], k_ref[m, 1, :, cols]
            real = real - (pr[m] * mr - pi[m] * mi)
            imag = imag - (pr[m] * mi + pi[m] * mr)
        vector_ref[0, :, cols] = real * scale
        vector_ref[1, :, cols] = imag * scale


def struct(*dims, dtype=F32):
    return pltpu.VMEM(dims, dtype)


def far(*dims, dtype=F32):
    return jax.ShapeDtypeStruct(dims, dtype)


def near(x):
    return pltpu.with_memory_space_constraint(x, pltpu.VMEM)


def call(kernel, out_shape, in_specs, flops, scratch=(), out_specs=None):
    single = not isinstance(out_shape, tuple)
    return pl.pallas_call(
        kernel,
        out_shape=out_shape,
        in_specs=in_specs,
        out_specs=out_specs or (VMEM if single else (VMEM,) * len(out_shape)),
        scratch_shapes=list(scratch),
        cost_estimate=pl.CostEstimate(flops=flops, bytes_accessed=1 << 20, transcendentals=0),
    )


def exchange(x, axes):
    return lax.all_to_all(x, axes, split_axis=0, concat_axis=0, tiled=True)


def per_device(krylov_basis, cond_time, capacity, diag_blocks, coupling, neighbours, pattern):
    h_dev = krylov_basis.shape[2]
    nodes_dev = krylov_basis.shape[3]
    blk = diag_blocks.shape[0]
    harm = lax.axis_size(HARM)
    groups = lax.axis_size(NODE)
    world = groups * harm
    names, present = neighbours.T, pattern.T
    krylov = near(krylov_basis)
    lanes = [pltpu.VMEM((LANES, LANES), F32)]

    packed = call(
        pack_kernel,
        far(blk, 4, h_dev, BS),
        [ANY, VMEM],
        1 << 20,
        [pltpu.VMEM((2, h_dev, nodes_dev), F32), pltpu.SemaphoreType.DMA],
    )(krylov_basis, cond_time)
    got = near(exchange(packed, HARM))
    hot_own = call(
        index_kernel, far(groups, LANES, dtype=jnp.int32), [SMEM, SMEM], 1 << 10, out_specs=SMEM
    )(names, present)
    hot = exchange(hot_own, NODE)
    turned = call(
        turn_kernel,
        struct(blk, BS, BS),
        [ANY],
        1 << 24,
        [pltpu.VMEM((blk, BS, BS), F32), pltpu.SemaphoreType.DMA((blk,))],
    )(diag_blocks)
    gram = call(gram_kernel, far(1, LANES), [VMEM], 1 << 24, lanes)(krylov)
    powers = 3
    means, solved = call(
        solve_kernel,
        (far(blk, BS), struct(blk, 2 * h_dev, BS)),
        [VMEM] * 3,
        1 << 31,
        [pltpu.VMEM((blk, powers, 2, BS, BS), BF16), pltpu.VMEM((blk, BS), F32)],
    )(got, near(turned), krylov)
    send_hot = call(
        select_kernel,
        far(groups, 2, 2 * h_dev, BS),
        [SMEM, VMEM],
        1 << 10,
        [pltpu.SemaphoreType.DMA((6, 2))],
        out_specs=ANY,
    )(hot, near(solved))
    named = near(exchange(send_hot, NODE))
    high, low = spectral_tables()
    send_cols = call(
        column_kernel,
        far(harm, 2, h_dev, BS),
        [VMEM, ANY] + [VMEM] * 4,
        1 << 27,
        [
            pltpu.VMEM((BS, BS), F32),
            pltpu.SemaphoreType.DMA,
            pltpu.VMEM((1, 2 * H, BS), F32),
            pltpu.VMEM((1, powers, 2, BS, BS), BF16),
        ],
    )(got, diag_blocks, means, capacity, jnp.asarray(high), jnp.asarray(low))
    back = near(exchange(send_cols, HARM))
    coupled = call(
        couple_kernel,
        struct(2, h_dev, nodes_dev),
        [SMEM] * 3 + [VMEM, ANY],
        1 << 28,
        [pltpu.VMEM(coupling.shape, F32), pltpu.SemaphoreType.DMA((blk,))],
    )(names, present, hot_own, named, coupling)
    image, send_sums = call(
        image_kernel,
        (struct(2, h_dev, nodes_dev), struct(world, LANES)),
        [VMEM] * 4,
        1 << 24,
        lanes,
    )(back, near(coupled), krylov, gram)
    sums = near(exchange(send_sums, NODE_HARM))
    count = world * h_dev * nodes_dev
    vector, proj, norm = call(
        lambda *refs: rest_kernel(count, *refs),
        (far(2, h_dev, nodes_dev), far(2, KRY), far(1, 1)),
        [VMEM] * 3,
        1 << 24,
    )(sums, near(image), krylov)
    return vector, proj, norm.reshape(())


def solution(mesh):
    finer = Mesh(mesh.devices.reshape(4, 4, 4, 2), ("node_0", "node_1", "harm_0", "harm_1"))
    placed = (
        P(None, None, HARM, NODE),
        P(HARM, NODE),
        P(NODE),
        P(NODE, None, None),
        P(NODE, None, None, None),
        P(NODE, None),
        P(NODE, None),
    )

    return jax.shard_map(
        per_device,
        mesh=finer,
        in_specs=placed,
        out_specs=(P(None, HARM, NODE), P(), P()),
        check_vma=False,
    )
```

```python
import math

import jax
import jax.numpy as jnp
import numpy as np
from jax import lax
from jax.experimental import pallas as pl
from jax.experimental.pallas import tpu as pltpu
from jax.sharding import Mesh
from jax.sharding import PartitionSpec as P

BS = 256
H = 64
NEIGH = 2
KRY = 8
HARM = ("harm_0", "harm_1")
NODE = ("node_0", "node_1")
NODE_HARM = ("node_0", "node_1", "harm_0", "harm_1")
F32 = jnp.float32
BF16 = jnp.bfloat16
LANES = 128
CODE = 16
OFFSETS = (1, 2, 3, -1, -2, -3)
GRAM = 64
SMEM = pl.BlockSpec(memory_space=pltpu.SMEM)
VMEM = pl.BlockSpec(memory_space=pltpu.VMEM)
ANY = pl.BlockSpec(memory_space=pl.ANY)


def spectral_tables():
    steps = np.arange(H)
    angles = (steps[:, None] * steps[None, :] % H) * (2.0 * math.pi / H)
    cosine = np.cos(angles) / math.sqrt(H)
    sine = np.sin(angles) / math.sqrt(H)
    table = np.block([[cosine, -sine], [sine, cosine]]).astype(np.float32)
    both = np.stack([table, table.T])
    high = both.astype(jnp.bfloat16)
    low = (both - high.astype(np.float32)).astype(jnp.bfloat16)
    return high, low


def split(x):
    high = x.astype(BF16)
    return high, (x - high.astype(F32)).astype(BF16)


def mm(a, b):
    return jnp.dot(a, b, preferred_element_type=F32)


def rows_mm(x, w_high, w_low, product=mm):
    rows = x.shape[0]
    high, low = split(x)
    both = product(jnp.concatenate([high, low], axis=0), w_high)
    return both[:rows] + both[rows:] + product(high, w_low)


def sublane_sum(x):
    return jnp.sum(x, axis=0, keepdims=True)


def rows_to_lanes(rows):
    return sublane_sum(jnp.transpose(rows))


def wide(ref, at, part):
    return jnp.concatenate([ref[at, 2 * part], ref[at, 2 * part + 1]], axis=1)


def pack_kernel(k_ref, cond_ref, out_ref, v, cond, sems):
    copies = [
        pltpu.make_async_copy(k_ref.at[KRY - 1], v, sems.at[0]),
        pltpu.make_async_copy(cond_ref, cond, sems.at[1]),
    ]
    for copy in copies:
        copy.start()
    for copy in copies:
        copy.wait()
    for b in range(out_ref.shape[0]):
        for t in range(2):
            cols = slice(BS * b + LANES * t, BS * b + LANES * (t + 1))
            out_ref[b, t] = v[0, :, cols]
            out_ref[b, 2 + t] = v[1, :, cols]
            out_ref[b, 4 + t] = cond[:, cols]


def turn_kernel(diag_ref, cap_ref, high_ref, low_ref, t_ref, cap_out, high_out, low_out, held, sem):
    copy = pltpu.make_async_copy(diag_ref.at[lax.axis_index(HARM)], held, sem)
    copy.start()
    cap_out[...] = cap_ref[...]
    high_out[...] = high_ref[...]
    low_out[...] = low_ref[...]
    copy.wait()
    t_ref[...] = jnp.transpose(held[...])


def gram_kernel(k_ref, gram_ref, rows):
    rows[...] = jnp.zeros_like(rows)
    chunks = k_ref.shape[3] // LANES
    for m in range(KRY):
        real = [None] * KRY
        imag = [None] * KRY
        for c in range(chunks):
            cols = slice(LANES * c, LANES * (c + 1))
            mr, mi = k_ref[m, 0, :, cols], k_ref[m, 1, :, cols]
            for n in range(m, KRY):
                nr, ni = (mr, mi) if n == m else (k_ref[n, 0, :, cols], k_ref[n, 1, :, cols])
                r = mr * nr + mi * ni
                real[n] = r if c == 0 else real[n] + r
                if n > m:
                    i = mr * ni - mi * nr
                    imag[n] = i if c == 0 else imag[n] + i
        for n in range(m, KRY):
            at = GRAM + KRY * m + n
            rows[at : at + 1] = sublane_sum(real[n])
            if n > m:
                at = GRAM + KRY * n + m
                rows[at : at + 1] = sublane_sum(imag[n])
    gram_ref[...] = rows_to_lanes(rows[...])


def named_code(names, blk):
    group = lax.div(names, blk)
    local = (names - group * blk).astype(F32)
    hit = (group == lax.axis_index(NODE)) & (names >= 0)

    def over_all(x, reduce):
        return reduce(reduce(x, axis=1, keepdims=True), axis=0, keepdims=True)

    least = over_all(jnp.where(hit, local, blk - 1.0), jnp.min)
    greatest = over_all(jnp.where(hit, local, 0.0), jnp.max)
    return jnp.broadcast_to(least * CODE + greatest, (8, LANES))


def column_kernel(got_ref, t_ref, cap_ref, high_ref, low_ref, names_ref, out_ref, e_ref):
    own = lax.axis_index(HARM)
    sources = got_ref.shape[0]
    powers = e_ref.shape[0]
    cond = jnp.concatenate([wide(got_ref, s, 2) for s in range(sources)], axis=0)
    mean = sublane_sum(cond) * (1.0 / H)
    d = 1.0 / mean
    u = jnp.concatenate([wide(got_ref, s, p) for p in range(2) for s in range(sources)], axis=0) * d
    power = t_ref[...] * (-d)
    for p in range(powers):
        e_ref[p, 0], e_ref[p, 1] = split(power)
        high, low = e_ref[p, 0], e_ref[p, 1]
        u = u + rows_mm(u, high, low)
        if p < powers - 1:
            power = mm(high, high) + mm(low, high) + mm(high, low)
    high, low = e_ref[powers - 1, 0], e_ref[powers - 1, 1]
    u = u + rows_mm(rows_mm(u, high, low), high, low)
    direct = rows_mm(u, e_ref[0, 0], e_ref[0, 1]) * (-mean)

    def transform(way, x):
        high, low = split(x)
        table = high_ref[way]
        return mm(table, high) + mm(table, low) + mm(low_ref[way], high)

    driven = transform(0, u) * jnp.concatenate([cond, cond], axis=0)
    image = direct + transform(1, driven)
    cap = cap_ref[pl.ds(pl.multiple_of(own * BS, BS), BS)].reshape(1, BS)
    harmonic = lax.broadcasted_iota(jnp.int32, (H, BS), 0)
    omega = jnp.where(harmonic < H // 2, harmonic, harmonic - H)
    react = omega.astype(F32) * cap
    real = image[:H] - react * u[H:]
    imag = image[H:] + react * u[:H]
    step = H // sources
    code = named_code(names_ref[...], sources)
    for s in range(sources):
        rows = slice(step * s, step * (s + 1))
        later = slice(H + step * s, H + step * (s + 1))
        for at, part in enumerate((real[rows], imag[rows], u[rows], u[later])):
            out_ref[s, 2 * at] = part[:, :LANES]
            out_ref[s, 2 * at + 1] = part[:, LANES:]
        out_ref[s, 8] = code


def select_kernel(back_ref, send_ref):
    me = lax.axis_index(NODE)
    groups = send_ref.shape[0]
    for at, offset in enumerate(OFFSETS):
        group = me - offset

        @pl.when((group >= 0) & (group < groups))
        def _():
            code = back_ref[at, 8, 0:1, 0:1][0, 0].astype(jnp.int32)
            least = lax.div(code, CODE)
            for slot, b in enumerate((least, code - least * CODE)):
                send_ref[group, slot] = back_ref[b, 4:8]


def halve_kernel(c_ref, near_ref, far_ref, held, halves, in_sems, out_sems):
    blk = held.shape[0]
    kept = near_ref.shape[0]
    order = [*range(kept, blk), *range(kept)]
    reads = [pltpu.make_async_copy(c_ref.at[b], held.at[b], in_sems.at[b]) for b in range(blk)]
    writes = {b: pltpu.make_async_copy(halves.at[b - kept], far_ref.at[b], out_sems.at[b - kept]) for b in order[: blk - kept]}
    for b in order:
        reads[b].start()
    for b in order:
        reads[b].wait()
        for j in range(NEIGH):
            high, low = split(jnp.transpose(held[b, j]))
            if b < kept:
                near_ref[b, j, 0], near_ref[b, j, 1] = high, low
            else:
                halves[b - kept, j, 0], halves[b - kept, j, 1] = high, low
        if b >= kept:
            writes[b].start()
    for write in writes.values():
        write.wait()


def image_kernel(
    names_ref, got_ref, near_ref, far_ref, back_ref, k_ref, gram_ref, image_ref, send_ref, least, rows, held, sems
):
    blk = names_ref.shape[1]
    kept = near_ref.shape[0]
    half = image_ref.shape[1]
    copies = {b: pltpu.make_async_copy(far_ref.at[b], held.at[b - kept], sems.at[b - kept]) for b in range(kept, blk)}
    for copy in copies.values():
        copy.start()
    for q in range(got_ref.shape[0]):
        least[q] = blk
    for j in range(NEIGH):
        for b in range(blk):
            name = names_ref[j, b]
            group = lax.div(name, blk)
            local = name - group * blk

            @pl.when(name >= 0)
            def _():
                least[group] = jnp.minimum(least[group], local)

    for b in range(blk):
        if b >= kept:
            copies[b].wait()
        halves, at = (near_ref, b) if b < kept else (held, b - kept)
        total = jnp.concatenate([wide(back_ref, b, 0), wide(back_ref, b, 1)], axis=0)
        for j in range(NEIGH):
            name = jnp.maximum(names_ref[j, b], 0)
            group = lax.div(name, blk)
            slot = jnp.where(name - group * blk == least[group], 0, 1)
            x = got_ref[group, slot]
            x = jnp.concatenate([jnp.concatenate([x[2 * p], x[2 * p + 1]], axis=1) for p in range(2)], axis=0)
            x = jnp.where(names_ref[j, b] >= 0, x, 0.0)
            total = total + rows_mm(x, halves[at, j, 0], halves[at, j, 1])
        cols = slice(b * BS, (b + 1) * BS)
        image_ref[0, :, cols] = total[:half]
        image_ref[1, :, cols] = total[half:]

    chunks = k_ref.shape[3] // LANES
    real = [None] * KRY
    imag = [None] * KRY
    squares = None
    for c in range(chunks):
        cols = slice(LANES * c, LANES * (c + 1))
        ir, ii = image_ref[0, :, cols], image_ref[1, :, cols]
        both = ir * ir + ii * ii
        squares = both if c == 0 else squares + both
        for m in range(KRY):
            mr, mi = k_ref[m, 0, :, cols], k_ref[m, 1, :, cols]
            r = mr * ir + mi * ii
            i = mr * ii - mi * ir
            real[m] = r if c == 0 else real[m] + r
            imag[m] = i if c == 0 else imag[m] + i
    rows[...] = jnp.zeros_like(rows)
    for m in range(KRY):
        rows[m : m + 1] = sublane_sum(real[m])
        rows[KRY + m : KRY + m + 1] = sublane_sum(imag[m])
    rows[2 * KRY : 2 * KRY + 1] = sublane_sum(squares)
    row = rows_to_lanes(rows[...]) + gram_ref[...]
    send_ref[...] = jnp.broadcast_to(row, send_ref.shape)


def rest_kernel(count, got_ref, image_ref, k_ref, vector_ref, proj_ref, norm_ref):
    totals = sublane_sum(got_ref[...]) * (1.0 / count)
    lane = lax.broadcasted_iota(jnp.int32, totals.shape, 1)

    def at(q):
        return jnp.broadcast_to(totals[:, q : q + 1], totals.shape)

    pr = [at(m) for m in range(KRY)]
    pi = [at(KRY + m) for m in range(KRY)]
    row_r = row_i = col_r = col_i = jnp.zeros_like(totals)
    row_of = (lane - GRAM) // KRY
    col_of = (lane - GRAM) - row_of * KRY
    for m in range(KRY):
        row_r = jnp.where(row_of == m, pr[m], row_r)
        row_i = jnp.where(row_of == m, pi[m], row_i)
        col_r = jnp.where(col_of == m, pr[m], col_r)
        col_i = jnp.where(col_of == m, pi[m], col_i)
    upper = row_r * col_r + row_i * col_i
    lower = col_i * row_r - col_r * row_i
    weight = jnp.where(row_of == col_of, upper, 2.0 * jnp.where(row_of < col_of, upper, lower))
    weight = jnp.where(lane >= GRAM, weight, 0.0)
    weight = jnp.where(lane < 2 * KRY, -2.0 * totals, weight)
    weight = jnp.where(lane == 2 * KRY, 1.0, weight)
    squares = jnp.sum(totals * weight, axis=1, keepdims=True)
    norm = jnp.sqrt(squares + 1e-06)
    norm_ref[...] = norm
    for m in range(KRY):
        proj_ref[0:1, m : m + 1] = pr[m][:, 0:1]
        proj_ref[1:2, m : m + 1] = pi[m][:, 0:1]
    half = k_ref.shape[2]
    scale = jnp.broadcast_to(1.0 / norm, (half, LANES))
    pr = [jnp.broadcast_to(x, (half, LANES)) for x in pr]
    pi = [jnp.broadcast_to(x, (half, LANES)) for x in pi]
    for c in range(k_ref.shape[3] // LANES):
        cols = slice(LANES * c, LANES * (c + 1))
        real, imag = image_ref[0, :, cols], image_ref[1, :, cols]
        for m in range(KRY):
            mr, mi = k_ref[m, 0, :, cols], k_ref[m, 1, :, cols]
            real = real - (pr[m] * mr - pi[m] * mi)
            imag = imag - (pr[m] * mi + pi[m] * mr)
        vector_ref[0, :, cols] = real * scale
        vector_ref[1, :, cols] = imag * scale


def struct(*dims, dtype=F32):
    return pltpu.VMEM(dims, dtype)


def far(*dims, dtype=F32):
    return jax.ShapeDtypeStruct(dims, dtype)


def near(x):
    return pltpu.with_memory_space_constraint(x, pltpu.VMEM)


def call(kernel, out_shape, in_specs, flops, scratch=(), out_specs=None, limit=60 * 1024 * 1024):
    single = not isinstance(out_shape, tuple)
    return pl.pallas_call(
        kernel,
        out_shape=out_shape,
        in_specs=in_specs,
        out_specs=out_specs or (VMEM if single else (VMEM,) * len(out_shape)),
        scratch_shapes=list(scratch),
        cost_estimate=pl.CostEstimate(flops=flops, bytes_accessed=1 << 20, transcendentals=0),
        compiler_params=pltpu.CompilerParams(vmem_limit_bytes=limit),
    )


def exchange(x, axes):
    return lax.all_to_all(x, axes, split_axis=0, concat_axis=0, tiled=True)


def per_device(krylov_basis, cond_time, capacity, diag_blocks, coupling, neighbours, pattern):
    h_dev = krylov_basis.shape[2]
    nodes_dev = krylov_basis.shape[3]
    blk = diag_blocks.shape[0]
    harm = lax.axis_size(HARM)
    groups = lax.axis_size(NODE)
    world = groups * harm
    names = jnp.where(pattern > 0, neighbours, -1).T
    lanes = [pltpu.VMEM((LANES, LANES), F32)]

    packed = call(
        pack_kernel,
        far(blk, 6, h_dev, LANES),
        [ANY, ANY],
        1 << 20,
        [
            pltpu.VMEM((2, h_dev, nodes_dev), F32),
            pltpu.VMEM((h_dev, nodes_dev), F32),
            pltpu.SemaphoreType.DMA((2,)),
        ],
    )(krylov_basis, cond_time)
    got = near(exchange(packed, HARM))
    pairs = [
        (g * harm + s, (g + offset) * harm + s)
        for s, offset in enumerate(OFFSETS)
        for g in range(groups)
        if 0 <= g + offset < groups
    ]
    named_by = lax.ppermute(names, NODE_HARM, pairs)
    high, low = spectral_tables()
    turned = call(
        turn_kernel,
        (
            struct(BS, BS),
            struct(*capacity.shape),
            struct(*high.shape, dtype=BF16),
            struct(*low.shape, dtype=BF16),
        ),
        [ANY] + [VMEM] * 3,
        1 << 24,
        [pltpu.VMEM((BS, BS), F32), pltpu.SemaphoreType.DMA],
    )(diag_blocks, capacity, jnp.asarray(high), jnp.asarray(low))
    send_cols = call(
        column_kernel,
        far(harm, 9, h_dev, LANES),
        [VMEM] * 6,
        1 << 29,
        [pltpu.VMEM((3, 2, BS, BS), BF16)],
    )(got, *map(near, turned), near(named_by))
    back = near(exchange(send_cols, HARM))
    send_named = call(select_kernel, struct(groups, 2, 4, h_dev, LANES), [VMEM], 1 << 10, limit=8 << 20)(back)
    named = near(exchange(near(send_named), NODE))
    gram = call(gram_kernel, far(1, LANES), [VMEM], 1 << 24, lanes)(krylov_basis)
    krylov = near(krylov_basis)
    kept = blk // 2
    room = 4 * blk
    near_halves, far_halves = call(
        halve_kernel,
        (
            struct(kept, NEIGH, 2, BS, BS, dtype=BF16),
            far(room, NEIGH, 2, BS, BS, dtype=BF16),
        ),
        [ANY],
        1 << 24,
        [
            pltpu.VMEM(coupling.shape, F32),
            pltpu.VMEM((blk - kept, NEIGH, 2, BS, BS), BF16),
            pltpu.SemaphoreType.DMA((blk,)),
            pltpu.SemaphoreType.DMA((blk - kept,)),
        ],
        out_specs=(VMEM, ANY),
    )(coupling)
    image, send_sums = call(
        image_kernel,
        (struct(2, h_dev, nodes_dev), struct(world, LANES)),
        [SMEM, VMEM, VMEM, ANY] + [VMEM] * 3,
        1 << 28,
        [
            pltpu.SMEM((groups,), jnp.int32),
            *lanes,
            pltpu.VMEM((blk - kept, NEIGH, 2, BS, BS), BF16),
            pltpu.SemaphoreType.DMA((blk - kept,)),
        ],
        limit=48 << 20,
    )(names, named, near(near_halves), far_halves, back, krylov, gram)
    sums = near(exchange(send_sums, NODE_HARM))
    count = world * h_dev * nodes_dev
    vector, proj, norm = call(
        lambda *refs: rest_kernel(count, *refs),
        (far(2, h_dev, nodes_dev), far(2, KRY), far(1, 1)),
        [VMEM] * 3,
        1 << 24,
        limit=48 << 20,
    )(sums, near(image), krylov)
    return vector, proj, norm.reshape(())


def solution(mesh):
    finer = Mesh(mesh.devices.reshape(4, 4, 4, 2), ("node_0", "node_1", "harm_0", "harm_1"))
    placed = (
        P(None, None, HARM, NODE),
        P(HARM, NODE),
        P(NODE),
        P(NODE, None, None),
        P(NODE, None, None, None),
        P(NODE, None),
        P(NODE, None),
    )

    return jax.shard_map(
        per_device,
        mesh=finer,
        in_specs=placed,
        out_specs=(P(None, HARM, NODE), P(), P()),
        check_vma=False,
    )
```

```python
import math

import jax
import jax.numpy as jnp
import numpy as np
from jax import lax
from jax.experimental import pallas as pl
from jax.experimental.pallas import tpu as pltpu
from jax.sharding import Mesh
from jax.sharding import PartitionSpec as P

BS = 256
H = 64
NEIGH = 2
KRY = 8
HARM = ("harm_0", "harm_1")
NODE = ("node_0", "node_1")
NODE_HARM = ("node_0", "node_1", "harm_0", "harm_1")
F32 = jnp.float32
BF16 = jnp.bfloat16
LANES = 128
CODE = 16
OFFSETS = (1, 2, 3, -1, -2, -3)
GRAM = 64
SMEM = pl.BlockSpec(memory_space=pltpu.SMEM)
VMEM = pl.BlockSpec(memory_space=pltpu.VMEM)
ANY = pl.BlockSpec(memory_space=pl.ANY)


def spectral_tables():
    steps = np.arange(H)
    angles = (steps[:, None] * steps[None, :] % H) * (2.0 * math.pi / H)
    cosine = np.cos(angles) / math.sqrt(H)
    sine = np.sin(angles) / math.sqrt(H)
    table = np.block([[cosine, -sine], [sine, cosine]]).astype(np.float32)
    both = np.stack([table, table.T])
    high = both.astype(jnp.bfloat16)
    low = (both - high.astype(np.float32)).astype(jnp.bfloat16)
    return high, low


def split(x):
    high = x.astype(BF16)
    return high, (x - high.astype(F32)).astype(BF16)


def mm(a, b):
    return jnp.dot(a, b, preferred_element_type=F32)


def rows_mm(x, w_high, w_low, product=mm):
    rows = x.shape[0]
    high, low = split(x)
    both = product(jnp.concatenate([high, low], axis=0), w_high)
    return both[:rows] + both[rows:] + product(high, w_low)


def sublane_sum(x):
    return jnp.sum(x, axis=0, keepdims=True)


def rows_to_lanes(rows):
    return sublane_sum(jnp.transpose(rows))


def wide(ref, at, part):
    return jnp.concatenate([ref[at, 2 * part], ref[at, 2 * part + 1]], axis=1)


def pack_kernel(k_ref, cond_ref, nb_ref, pat_ref, out_ref, names_ref, v, cond, nb, pat, sems):
    copies = [
        pltpu.make_async_copy(source, target, sems.at[at])
        for at, (source, target) in enumerate(
            ((k_ref.at[KRY - 1], v), (cond_ref, cond), (nb_ref, nb), (pat_ref, pat))
        )
    ]
    for copy in copies:
        copy.start()
    for copy in copies:
        copy.wait()
    names_ref[...] = jnp.where(pat[...] > 0, nb[...], -1)
    for b in range(out_ref.shape[0]):
        for t in range(2):
            cols = slice(BS * b + LANES * t, BS * b + LANES * (t + 1))
            out_ref[b, t] = v[0, :, cols]
            out_ref[b, 2 + t] = v[1, :, cols]
            out_ref[b, 4 + t] = cond[:, cols]


def turn_kernel(diag_ref, cap_ref, high_ref, low_ref, t_ref, cap_out, high_out, low_out, held, sem):
    copy = pltpu.make_async_copy(diag_ref.at[lax.axis_index(HARM)], held, sem)
    copy.start()
    cap_out[...] = cap_ref[...]
    high_out[...] = high_ref[...]
    low_out[...] = low_ref[...]
    copy.wait()
    t_ref[...] = jnp.transpose(held[...])


def gram_kernel(k_ref, gram_ref, rows):
    rows[...] = jnp.zeros_like(rows)
    chunks = k_ref.shape[3] // LANES
    for m in range(KRY):
        real = [None] * KRY
        imag = [None] * KRY
        for c in range(chunks):
            cols = slice(LANES * c, LANES * (c + 1))
            mr, mi = k_ref[m, 0, :, cols], k_ref[m, 1, :, cols]
            for n in range(m, KRY):
                nr, ni = (mr, mi) if n == m else (k_ref[n, 0, :, cols], k_ref[n, 1, :, cols])
                r = mr * nr + mi * ni
                real[n] = r if c == 0 else real[n] + r
                if n > m:
                    i = mr * ni - mi * nr
                    imag[n] = i if c == 0 else imag[n] + i
        for n in range(m, KRY):
            at = GRAM + KRY * m + n
            rows[at : at + 1] = sublane_sum(real[n])
            if n > m:
                at = GRAM + KRY * n + m
                rows[at : at + 1] = sublane_sum(imag[n])
    gram_ref[...] = rows_to_lanes(rows[...])


def named_code(names, blk):
    group = lax.div(names, blk)
    local = (names - group * blk).astype(F32)
    hit = (group == lax.axis_index(NODE)) & (names >= 0)

    def over_all(x, reduce):
        return reduce(reduce(x, axis=1, keepdims=True), axis=0, keepdims=True)

    least = over_all(jnp.where(hit, local, blk - 1.0), jnp.min)
    greatest = over_all(jnp.where(hit, local, 0.0), jnp.max)
    return jnp.broadcast_to(least * CODE + greatest, (8, LANES))


def solve_kernel(got_ref, t_ref, u_ref, direct_ref, e_ref):
    sources = got_ref.shape[0]
    powers = e_ref.shape[0]
    mean = sublane_sum(conductance(got_ref)) * (1.0 / H)
    d = 1.0 / mean
    u = jnp.concatenate([wide(got_ref, s, p) for p in range(2) for s in range(sources)], axis=0) * d
    power = t_ref[...] * (-d)
    for p in range(powers):
        e_ref[p, 0], e_ref[p, 1] = split(power)
        high, low = e_ref[p, 0], e_ref[p, 1]
        u = u + rows_mm(u, high, low)
        if p < powers - 1:
            power = mm(high, high) + mm(low, high) + mm(high, low)
    high, low = e_ref[powers - 1, 0], e_ref[powers - 1, 1]
    u = u + rows_mm(rows_mm(u, high, low), high, low)
    u_ref[...] = u
    direct_ref[...] = rows_mm(u, e_ref[0, 0], e_ref[0, 1]) * (-mean)


def conductance(got_ref):
    return jnp.concatenate([wide(got_ref, s, 2) for s in range(got_ref.shape[0])], axis=0)


def column_kernel(got_ref, u_ref, direct_ref, cap_ref, high_ref, low_ref, names_ref, out_ref):
    own = lax.axis_index(HARM)
    sources = got_ref.shape[0]
    u = u_ref[...]
    cond = conductance(got_ref)

    def transform(way, x):
        high, low = split(x)
        table = high_ref[way]
        return mm(table, high) + mm(table, low) + mm(low_ref[way], high)

    driven = transform(0, u) * jnp.concatenate([cond, cond], axis=0)
    image = direct_ref[...] + transform(1, driven)
    cap = cap_ref[pl.ds(pl.multiple_of(own * BS, BS), BS)].reshape(1, BS)
    harmonic = lax.broadcasted_iota(jnp.int32, (H, BS), 0)
    omega = jnp.where(harmonic < H // 2, harmonic, harmonic - H)
    react = omega.astype(F32) * cap
    real = image[:H] - react * u[H:]
    imag = image[H:] + react * u[:H]
    step = H // sources
    code = named_code(names_ref[...], sources)
    for s in range(sources):
        rows = slice(step * s, step * (s + 1))
        later = slice(H + step * s, H + step * (s + 1))
        for at, part in enumerate((real[rows], imag[rows], u[rows], u[later])):
            out_ref[s, 2 * at] = part[:, :LANES]
            out_ref[s, 2 * at + 1] = part[:, LANES:]
        out_ref[s, 8] = code


def pass_kernel(back_ref, halves_ref, mark_ref, passed_ref):
    del halves_ref, passed_ref
    mark_ref[...] = back_ref[0, 8]


def select_kernel(back_ref, mark_ref, send_ref):
    del mark_ref
    me = lax.axis_index(NODE)
    groups = send_ref.shape[0]
    for at, offset in enumerate(OFFSETS):
        group = me - offset

        @pl.when((group >= 0) & (group < groups))
        def _():
            code = back_ref[at, 8, 0:1, 0:1][0, 0].astype(jnp.int32)
            least = lax.div(code, CODE)
            for slot, b in enumerate((least, code - least * CODE)):
                send_ref[group, slot] = back_ref[b, 4:8]


def halve_kernel(c_ref, out_ref, held, halves, in_sems, out_sems):
    blk = held.shape[0]
    reads = [pltpu.make_async_copy(c_ref.at[b], held.at[b], in_sems.at[b]) for b in range(blk)]
    writes = [pltpu.make_async_copy(halves.at[b], out_ref.at[b], out_sems.at[b]) for b in range(blk)]
    for read in reads:
        read.start()
    for b in range(blk):
        reads[b].wait()
        for j in range(NEIGH):
            halves[b, j, 0], halves[b, j, 1] = split(jnp.transpose(held[b, j]))
        writes[b].start()
    for write in writes:
        write.wait()


def image_kernel(names_ref, got_ref, halves_ref, back_ref, k_ref, gram_ref, image_ref, send_ref, least, rows):
    blk = halves_ref.shape[0]
    half = image_ref.shape[1]
    for q in range(got_ref.shape[0]):
        least[q] = blk
    for j in range(NEIGH):
        for b in range(blk):
            name = names_ref[j, b]
            group = lax.div(name, blk)
            local = name - group * blk

            @pl.when(name >= 0)
            def _():
                least[group] = jnp.minimum(least[group], local)

    for b in range(blk):
        total = jnp.concatenate([wide(back_ref, b, 0), wide(back_ref, b, 1)], axis=0)
        for j in range(NEIGH):
            name = jnp.maximum(names_ref[j, b], 0)
            group = lax.div(name, blk)
            slot = jnp.where(name - group * blk == least[group], 0, 1)
            x = got_ref[group, slot]
            x = jnp.concatenate([jnp.concatenate([x[2 * p], x[2 * p + 1]], axis=1) for p in range(2)], axis=0)
            x = jnp.where(names_ref[j, b] >= 0, x, 0.0)
            total = total + rows_mm(x, halves_ref[b, j, 0], halves_ref[b, j, 1])
        cols = slice(b * BS, (b + 1) * BS)
        image_ref[0, :, cols] = total[:half]
        image_ref[1, :, cols] = total[half:]

    chunks = k_ref.shape[3] // LANES
    real = [None] * KRY
    imag = [None] * KRY
    squares = None
    for c in range(chunks):
        cols = slice(LANES * c, LANES * (c + 1))
        ir, ii = image_ref[0, :, cols], image_ref[1, :, cols]
        both = ir * ir + ii * ii
        squares = both if c == 0 else squares + both
        for m in range(KRY):
            mr, mi = k_ref[m, 0, :, cols], k_ref[m, 1, :, cols]
            r = mr * ir + mi * ii
            i = mr * ii - mi * ir
            real[m] = r if c == 0 else real[m] + r
            imag[m] = i if c == 0 else imag[m] + i
    rows[...] = jnp.zeros_like(rows)
    for m in range(KRY):
        rows[m : m + 1] = sublane_sum(real[m])
        rows[KRY + m : KRY + m + 1] = sublane_sum(imag[m])
    rows[2 * KRY : 2 * KRY + 1] = sublane_sum(squares)
    row = rows_to_lanes(rows[...]) + gram_ref[...]
    send_ref[...] = jnp.broadcast_to(row, send_ref.shape)


def rest_kernel(count, got_ref, image_ref, k_ref, vector_ref, proj_ref, norm_ref):
    totals = sublane_sum(got_ref[...]) * (1.0 / count)
    lane = lax.broadcasted_iota(jnp.int32, totals.shape, 1)

    def at(q):
        return jnp.broadcast_to(totals[:, q : q + 1], totals.shape)

    pr = [at(m) for m in range(KRY)]
    pi = [at(KRY + m) for m in range(KRY)]
    row_r = row_i = col_r = col_i = jnp.zeros_like(totals)
    row_of = (lane - GRAM) // KRY
    col_of = (lane - GRAM) - row_of * KRY
    for m in range(KRY):
        row_r = jnp.where(row_of == m, pr[m], row_r)
        row_i = jnp.where(row_of == m, pi[m], row_i)
        col_r = jnp.where(col_of == m, pr[m], col_r)
        col_i = jnp.where(col_of == m, pi[m], col_i)
    upper = row_r * col_r + row_i * col_i
    lower = col_i * row_r - col_r * row_i
    weight = jnp.where(row_of == col_of, upper, 2.0 * jnp.where(row_of < col_of, upper, lower))
    weight = jnp.where(lane >= GRAM, weight, 0.0)
    weight = jnp.where(lane < 2 * KRY, -2.0 * totals, weight)
    weight = jnp.where(lane == 2 * KRY, 1.0, weight)
    squares = jnp.sum(totals * weight, axis=1, keepdims=True)
    norm = jnp.sqrt(squares + 1e-06)
    norm_ref[...] = norm
    for m in range(KRY):
        proj_ref[0:1, m : m + 1] = pr[m][:, 0:1]
        proj_ref[1:2, m : m + 1] = pi[m][:, 0:1]
    half = k_ref.shape[2]
    scale = jnp.broadcast_to(1.0 / norm, (half, LANES))
    pr = [jnp.broadcast_to(x, (half, LANES)) for x in pr]
    pi = [jnp.broadcast_to(x, (half, LANES)) for x in pi]
    for c in range(k_ref.shape[3] // LANES):
        cols = slice(LANES * c, LANES * (c + 1))
        real, imag = image_ref[0, :, cols], image_ref[1, :, cols]
        for m in range(KRY):
            mr, mi = k_ref[m, 0, :, cols], k_ref[m, 1, :, cols]
            real = real - (pr[m] * mr - pi[m] * mi)
            imag = imag - (pr[m] * mi + pi[m] * mr)
        vector_ref[0, :, cols] = real * scale
        vector_ref[1, :, cols] = imag * scale


def struct(*dims, dtype=F32):
    return pltpu.VMEM(dims, dtype)


def far(*dims, dtype=F32):
    return jax.ShapeDtypeStruct(dims, dtype)


def near(x):
    return pltpu.with_memory_space_constraint(x, pltpu.VMEM)


def call(kernel, out_shape, in_specs, flops, scratch=(), out_specs=None, limit=60 * 1024 * 1024, aliases=None):
    single = not isinstance(out_shape, tuple)
    return pl.pallas_call(
        kernel,
        out_shape=out_shape,
        in_specs=in_specs,
        out_specs=out_specs or (VMEM if single else (VMEM,) * len(out_shape)),
        scratch_shapes=list(scratch),
        cost_estimate=pl.CostEstimate(flops=flops, bytes_accessed=1 << 20, transcendentals=0),
        compiler_params=pltpu.CompilerParams(vmem_limit_bytes=limit),
        input_output_aliases=aliases or {},
    )


def exchange(x, axes):
    return lax.all_to_all(x, axes, split_axis=0, concat_axis=0, tiled=True)


def per_device(krylov_basis, cond_time, capacity, diag_blocks, coupling, neighbours, pattern):
    h_dev = krylov_basis.shape[2]
    nodes_dev = krylov_basis.shape[3]
    blk = diag_blocks.shape[0]
    harm = lax.axis_size(HARM)
    groups = lax.axis_size(NODE)
    world = groups * harm
    lanes = [pltpu.VMEM((LANES, LANES), F32)]
    krylov = near(krylov_basis)

    packed, names = call(
        pack_kernel,
        (far(blk, 6, h_dev, LANES), far(NEIGH, blk, dtype=jnp.int32)),
        [ANY] * 4,
        1 << 20,
        [
            pltpu.VMEM((2, h_dev, nodes_dev), F32),
            pltpu.VMEM((h_dev, nodes_dev), F32),
            pltpu.VMEM((NEIGH, blk), jnp.int32),
            pltpu.VMEM((NEIGH, blk), jnp.int32),
            pltpu.SemaphoreType.DMA((4,)),
        ],
    )(krylov_basis, cond_time, neighbours.T, pattern.T)
    got = near(exchange(packed, HARM))
    pairs = [
        (g * harm + s, (g + offset) * harm + s)
        for s, offset in enumerate(OFFSETS)
        for g in range(groups)
        if 0 <= g + offset < groups
    ]
    named_by = lax.ppermute(names, NODE_HARM, pairs)
    high, low = spectral_tables()
    turned = call(
        turn_kernel,
        (
            struct(BS, BS),
            struct(*capacity.shape),
            struct(*high.shape, dtype=BF16),
            struct(*low.shape, dtype=BF16),
        ),
        [ANY] + [VMEM] * 3,
        1 << 24,
        [pltpu.VMEM((BS, BS), F32), pltpu.SemaphoreType.DMA],
    )(diag_blocks, capacity, jnp.asarray(high), jnp.asarray(low))
    turned, *tables = turned
    solved, direct = call(
        solve_kernel,
        (struct(2 * H, BS), struct(2 * H, BS)),
        [VMEM] * 2,
        1 << 29,
        [pltpu.VMEM((3, 2, BS, BS), BF16)],
    )(got, near(turned))
    send_cols = call(column_kernel, far(harm, 9, h_dev, LANES), [VMEM] * 7, 1 << 27)(
        got, near(solved), near(direct), *map(near, tables), near(named_by)
    )
    back = near(exchange(send_cols, HARM))
    halves = call(
        halve_kernel,
        far(blk, NEIGH, 2, BS, BS, dtype=BF16),
        [ANY],
        1 << 24,
        [
            pltpu.VMEM(coupling.shape, F32),
            pltpu.VMEM((blk, NEIGH, 2, BS, BS), BF16),
            pltpu.SemaphoreType.DMA((blk,)),
            pltpu.SemaphoreType.DMA((blk,)),
        ],
        out_specs=ANY,
    )(coupling)
    mark, halves = call(
        pass_kernel,
        (struct(h_dev, LANES), far(*halves.shape, dtype=BF16)),
        [VMEM, ANY],
        1 << 10,
        out_specs=(VMEM, ANY),
        aliases={1: 1},
    )(back, halves)
    send_named = call(
        select_kernel, struct(groups, 2, 4, h_dev, LANES), [VMEM, VMEM], 1 << 34, limit=32 << 20
    )(back, near(mark))
    named = near(exchange(near(send_named), NODE))
    gram = call(gram_kernel, far(1, LANES), [VMEM], 1 << 24, lanes)(krylov)
    image, send_sums = call(
        image_kernel,
        (struct(2, h_dev, nodes_dev), struct(world, LANES)),
        [SMEM] + [VMEM] * 5,
        1 << 28,
        [pltpu.SMEM((groups,), jnp.int32), *lanes],
        limit=32 << 20,
    )(names, named, near(halves), back, krylov, gram)
    sums = near(exchange(send_sums, NODE_HARM))
    count = world * h_dev * nodes_dev
    vector, proj, norm = call(
        lambda *refs: rest_kernel(count, *refs),
        (far(2, h_dev, nodes_dev), far(2, KRY), far(1, 1)),
        [VMEM] * 3,
        1 << 24,
        limit=48 << 20,
    )(sums, near(image), krylov)
    return vector, proj, norm.reshape(())


def solution(mesh):
    finer = Mesh(mesh.devices.reshape(4, 4, 4, 2), ("node_0", "node_1", "harm_0", "harm_1"))
    placed = (
        P(None, None, HARM, NODE),
        P(HARM, NODE),
        P(NODE),
        P(NODE, None, None),
        P(NODE, None, None, None),
        P(NODE, None),
        P(NODE, None),
    )

    return jax.shard_map(
        per_device,
        mesh=finer,
        in_specs=placed,
        out_specs=(P(None, HARM, NODE), P(), P()),
        check_vma=False,
    )
```

```python
import math

import jax
import jax.numpy as jnp
import numpy as np
from jax import lax
from jax.experimental import pallas as pl
from jax.experimental.pallas import tpu as pltpu
from jax.sharding import Mesh
from jax.sharding import PartitionSpec as P

BS = 256
H = 64
NEIGH = 2
KRY = 8
HARM = ("harm_0", "harm_1")
NODE = ("node_0", "node_1")
NODE_HARM = ("node_0", "node_1", "harm_0", "harm_1")
F32 = jnp.float32
BF16 = jnp.bfloat16
LANES = 128
CODE = 16
OFFSETS = (1, 2, 3, -1, -2, -3)
GRAM = 64
SMEM = pl.BlockSpec(memory_space=pltpu.SMEM)
VMEM = pl.BlockSpec(memory_space=pltpu.VMEM)
ANY = pl.BlockSpec(memory_space=pl.ANY)


def spectral_tables():
    steps = np.arange(H)
    angles = (steps[:, None] * steps[None, :] % H) * (2.0 * math.pi / H)
    cosine = np.cos(angles) / math.sqrt(H)
    sine = np.sin(angles) / math.sqrt(H)
    table = np.block([[cosine, -sine], [sine, cosine]]).astype(np.float32)
    both = np.stack([table, table.T])
    high = both.astype(jnp.bfloat16)
    low = (both - high.astype(np.float32)).astype(jnp.bfloat16)
    return high, low


def split(x):
    high = x.astype(BF16)
    return high, (x - high.astype(F32)).astype(BF16)


def mm(a, b):
    return jnp.dot(a, b, preferred_element_type=F32)


def rows_mm(x, w_high, w_low, product=mm):
    rows = x.shape[0]
    high, low = split(x)
    both = product(jnp.concatenate([high, low], axis=0), w_high)
    return both[:rows] + both[rows:] + product(high, w_low)


def sublane_sum(x):
    return jnp.sum(x, axis=0, keepdims=True)


def rows_to_lanes(rows):
    return sublane_sum(jnp.transpose(rows))


def wide(ref, at, part):
    return jnp.concatenate([ref[at, 2 * part], ref[at, 2 * part + 1]], axis=1)


def pack_kernel(k_ref, cond_ref, nb_ref, pat_ref, out_ref, names_ref, v, cond, nb, pat, sems):
    copies = [
        pltpu.make_async_copy(source, target, sems.at[at])
        for at, (source, target) in enumerate(
            ((k_ref.at[KRY - 1], v), (cond_ref, cond), (nb_ref, nb), (pat_ref, pat))
        )
    ]
    for copy in copies:
        copy.start()
    for copy in copies:
        copy.wait()
    names_ref[...] = jnp.where(pat[...] > 0, nb[...], -1)
    for b in range(out_ref.shape[0]):
        for t in range(2):
            cols = slice(BS * b + LANES * t, BS * b + LANES * (t + 1))
            out_ref[b, t] = v[0, :, cols]
            out_ref[b, 2 + t] = v[1, :, cols]
            out_ref[b, 4 + t] = cond[:, cols]


def turn_kernel(
    names_ref, diag_ref, cap_ref, high_ref, low_ref, t_ref, where_ref, cap_out, high_out, low_out, held, names, least, sems
):
    copies = [
        pltpu.make_async_copy(source, target, sems.at[at])
        for at, (source, target) in enumerate(
            (
                (diag_ref.at[lax.axis_index(HARM)], held),
                (names_ref, names),
                (cap_ref, cap_out),
                (high_ref, high_out),
                (low_ref, low_out),
            )
        )
    ]
    for copy in copies:
        copy.start()
    copies[1].wait()
    blk = names.shape[1]
    for q in range(least.shape[0]):
        least[q] = blk
    for j in range(NEIGH):
        for b in range(blk):
            name = names[j, b]
            group = lax.div(name, blk)
            local = name - group * blk

            @pl.when(name >= 0)
            def _():
                least[group] = jnp.minimum(least[group], local)

    for j in range(NEIGH):
        for b in range(blk):
            name = names[j, b]
            group = lax.div(jnp.maximum(name, 0), blk)
            slot = jnp.where(name - group * blk == least[group], 0, 1)
            where_ref[j, b] = jnp.where(name >= 0, 2 * group + slot, -1)
    copies[0].wait()
    t_ref[...] = jnp.transpose(held[...])
    for copy in copies[2:]:
        copy.wait()


def gram_kernel(k_ref, gram_ref, rows):
    rows[...] = jnp.zeros_like(rows)
    chunks = k_ref.shape[3] // LANES
    for m in range(KRY):
        real = [None] * KRY
        imag = [None] * KRY
        for c in range(chunks):
            cols = slice(LANES * c, LANES * (c + 1))
            mr, mi = k_ref[m, 0, :, cols], k_ref[m, 1, :, cols]
            for n in range(m, KRY):
                nr, ni = (mr, mi) if n == m else (k_ref[n, 0, :, cols], k_ref[n, 1, :, cols])
                r = mr * nr + mi * ni
                real[n] = r if c == 0 else real[n] + r
                if n > m:
                    i = mr * ni - mi * nr
                    imag[n] = i if c == 0 else imag[n] + i
        for n in range(m, KRY):
            at = GRAM + KRY * m + n
            rows[at : at + 1] = sublane_sum(real[n])
            if n > m:
                at = GRAM + KRY * n + m
                rows[at : at + 1] = sublane_sum(imag[n])
    gram_ref[...] = rows_to_lanes(rows[...])


def named_code(names, blk):
    group = lax.div(names, blk)
    local = (names - group * blk).astype(F32)
    hit = (group == lax.axis_index(NODE)) & (names >= 0)

    def over_all(x, reduce):
        return reduce(reduce(x, axis=1, keepdims=True), axis=0, keepdims=True)

    least = over_all(jnp.where(hit, local, blk - 1.0), jnp.min)
    greatest = over_all(jnp.where(hit, local, 0.0), jnp.max)
    return jnp.broadcast_to(least * CODE + greatest, (8, LANES))


def solve_kernel(got_ref, t_ref, u_ref, direct_ref, e_ref):
    sources = got_ref.shape[0]
    powers = e_ref.shape[0]
    mean = sublane_sum(conductance(got_ref)) * (1.0 / H)
    d = 1.0 / mean
    u = jnp.concatenate([wide(got_ref, s, p) for p in range(2) for s in range(sources)], axis=0) * d
    power = t_ref[...] * (-d)
    for p in range(powers):
        e_ref[p, 0], e_ref[p, 1] = split(power)
        high, low = e_ref[p, 0], e_ref[p, 1]
        u = u + rows_mm(u, high, low)
        if p < powers - 1:
            power = mm(high, high) + mm(low, high) + mm(high, low)
    high, low = e_ref[powers - 1, 0], e_ref[powers - 1, 1]
    u = u + rows_mm(rows_mm(u, high, low), high, low)
    u_ref[...] = u
    direct_ref[...] = rows_mm(u, e_ref[0, 0], e_ref[0, 1]) * (-mean)


def conductance(got_ref):
    return jnp.concatenate([wide(got_ref, s, 2) for s in range(got_ref.shape[0])], axis=0)


def column_kernel(got_ref, u_ref, direct_ref, cap_ref, high_ref, low_ref, names_ref, out_ref):
    own = lax.axis_index(HARM)
    sources = got_ref.shape[0]
    u = u_ref[...]
    cond = conductance(got_ref)

    def transform(way, x):
        high, low = split(x)
        table = high_ref[way]
        return mm(table, high) + mm(table, low) + mm(low_ref[way], high)

    driven = transform(0, u) * jnp.concatenate([cond, cond], axis=0)
    image = direct_ref[...] + transform(1, driven)
    cap = cap_ref[pl.ds(pl.multiple_of(own * BS, BS), BS)].reshape(1, BS)
    harmonic = lax.broadcasted_iota(jnp.int32, (H, BS), 0)
    omega = jnp.where(harmonic < H // 2, harmonic, harmonic - H)
    react = omega.astype(F32) * cap
    real = image[:H] - react * u[H:]
    imag = image[H:] + react * u[:H]
    step = H // sources
    code = named_code(names_ref[...], sources)
    for s in range(sources):
        rows = slice(step * s, step * (s + 1))
        later = slice(H + step * s, H + step * (s + 1))
        for at, part in enumerate((real[rows], imag[rows], u[rows], u[later])):
            out_ref[s, 2 * at] = part[:, :LANES]
            out_ref[s, 2 * at + 1] = part[:, LANES:]
        out_ref[s, 8] = code


def select_kernel(back_ref, send_ref):
    me = lax.axis_index(NODE)
    groups = send_ref.shape[0]
    for at, offset in enumerate(OFFSETS):
        group = me - offset

        @pl.when((group >= 0) & (group < groups))
        def _():
            code = back_ref[at, 8, 0:1, 0:1][0, 0].astype(jnp.int32)
            least = lax.div(code, CODE)
            for slot, b in enumerate((least, code - least * CODE)):
                send_ref[group, slot] = back_ref[b, 4:8]


def halve_kernel(c_ref, out_ref, held, halves, in_sems, out_sems):
    blk = held.shape[0]
    reads = [pltpu.make_async_copy(c_ref.at[b], held.at[b], in_sems.at[b]) for b in range(blk)]
    writes = [pltpu.make_async_copy(halves.at[b], out_ref.at[b], out_sems.at[b]) for b in range(blk)]
    for read in reads:
        read.start()
    for b in range(blk):
        reads[b].wait()
        for j in range(NEIGH):
            halves[b, j, 0], halves[b, j, 1] = split(jnp.transpose(held[b, j]))
        writes[b].start()
    for write in writes:
        write.wait()


def image_kernel(where_ref, got_ref, halves_ref, back_ref, k_ref, gram_ref, image_ref, send_ref, rows):
    blk = halves_ref.shape[0]
    half = image_ref.shape[1]
    for b in range(blk):
        total = jnp.concatenate([wide(back_ref, b, 0), wide(back_ref, b, 1)], axis=0)
        for j in range(NEIGH):
            at = where_ref[j : j + 1, b : b + 1][0, 0]
            group = lax.div(jnp.maximum(at, 0), 2)
            x = got_ref[group, jnp.maximum(at - 2 * group, 0)]
            x = jnp.concatenate([jnp.concatenate([x[2 * p], x[2 * p + 1]], axis=1) for p in range(2)], axis=0)
            x = jnp.where(at >= 0, x, 0.0)
            total = total + rows_mm(x, halves_ref[b, j, 0], halves_ref[b, j, 1])
        cols = slice(b * BS, (b + 1) * BS)
        image_ref[0, :, cols] = total[:half]
        image_ref[1, :, cols] = total[half:]

    chunks = k_ref.shape[3] // LANES
    real = [None] * KRY
    imag = [None] * KRY
    squares = None
    for c in range(chunks):
        cols = slice(LANES * c, LANES * (c + 1))
        ir, ii = image_ref[0, :, cols], image_ref[1, :, cols]
        both = ir * ir + ii * ii
        squares = both if c == 0 else squares + both
        for m in range(KRY):
            mr, mi = k_ref[m, 0, :, cols], k_ref[m, 1, :, cols]
            r = mr * ir + mi * ii
            i = mr * ii - mi * ir
            real[m] = r if c == 0 else real[m] + r
            imag[m] = i if c == 0 else imag[m] + i
    rows[...] = jnp.zeros_like(rows)
    for m in range(KRY):
        rows[m : m + 1] = sublane_sum(real[m])
        rows[KRY + m : KRY + m + 1] = sublane_sum(imag[m])
    rows[2 * KRY : 2 * KRY + 1] = sublane_sum(squares)
    row = rows_to_lanes(rows[...]) + gram_ref[...]
    send_ref[...] = jnp.broadcast_to(row, send_ref.shape)


def rest_kernel(count, got_ref, image_ref, k_ref, vector_ref, proj_ref, norm_ref):
    totals = sublane_sum(got_ref[...]) * (1.0 / count)
    lane = lax.broadcasted_iota(jnp.int32, totals.shape, 1)

    def at(q):
        return jnp.broadcast_to(totals[:, q : q + 1], totals.shape)

    pr = [at(m) for m in range(KRY)]
    pi = [at(KRY + m) for m in range(KRY)]
    row_r = row_i = col_r = col_i = jnp.zeros_like(totals)
    row_of = (lane - GRAM) // KRY
    col_of = (lane - GRAM) - row_of * KRY
    for m in range(KRY):
        row_r = jnp.where(row_of == m, pr[m], row_r)
        row_i = jnp.where(row_of == m, pi[m], row_i)
        col_r = jnp.where(col_of == m, pr[m], col_r)
        col_i = jnp.where(col_of == m, pi[m], col_i)
    upper = row_r * col_r + row_i * col_i
    lower = col_i * row_r - col_r * row_i
    weight = jnp.where(row_of == col_of, upper, 2.0 * jnp.where(row_of < col_of, upper, lower))
    weight = jnp.where(lane >= GRAM, weight, 0.0)
    weight = jnp.where(lane < 2 * KRY, -2.0 * totals, weight)
    weight = jnp.where(lane == 2 * KRY, 1.0, weight)
    squares = jnp.sum(totals * weight, axis=1, keepdims=True)
    norm = jnp.sqrt(squares + 1e-06)
    norm_ref[...] = norm
    for m in range(KRY):
        proj_ref[0:1, m : m + 1] = pr[m][:, 0:1]
        proj_ref[1:2, m : m + 1] = pi[m][:, 0:1]
    half = k_ref.shape[2]
    scale = jnp.broadcast_to(1.0 / norm, (half, LANES))
    pr = [jnp.broadcast_to(x, (half, LANES)) for x in pr]
    pi = [jnp.broadcast_to(x, (half, LANES)) for x in pi]
    for c in range(k_ref.shape[3] // LANES):
        cols = slice(LANES * c, LANES * (c + 1))
        real, imag = image_ref[0, :, cols], image_ref[1, :, cols]
        for m in range(KRY):
            mr, mi = k_ref[m, 0, :, cols], k_ref[m, 1, :, cols]
            real = real - (pr[m] * mr - pi[m] * mi)
            imag = imag - (pr[m] * mi + pi[m] * mr)
        vector_ref[0, :, cols] = real * scale
        vector_ref[1, :, cols] = imag * scale


def struct(*dims, dtype=F32):
    return pltpu.VMEM(dims, dtype)


def far(*dims, dtype=F32):
    return jax.ShapeDtypeStruct(dims, dtype)


def near(x):
    return pltpu.with_memory_space_constraint(x, pltpu.VMEM)


def call(kernel, out_shape, in_specs, flops, scratch=(), out_specs=None, limit=60 * 1024 * 1024, aliases=None):
    single = not isinstance(out_shape, tuple)
    return pl.pallas_call(
        kernel,
        out_shape=out_shape,
        in_specs=in_specs,
        out_specs=out_specs or (VMEM if single else (VMEM,) * len(out_shape)),
        scratch_shapes=list(scratch),
        cost_estimate=pl.CostEstimate(flops=flops, bytes_accessed=1 << 20, transcendentals=0),
        compiler_params=pltpu.CompilerParams(vmem_limit_bytes=limit),
        input_output_aliases=aliases or {},
    )


def exchange(x, axes):
    return lax.all_to_all(x, axes, split_axis=0, concat_axis=0, tiled=True)


def per_device(krylov_basis, cond_time, capacity, diag_blocks, coupling, neighbours, pattern):
    h_dev = krylov_basis.shape[2]
    nodes_dev = krylov_basis.shape[3]
    blk = diag_blocks.shape[0]
    harm = lax.axis_size(HARM)
    groups = lax.axis_size(NODE)
    world = groups * harm
    lanes = [pltpu.VMEM((LANES, LANES), F32)]
    krylov = near(krylov_basis)

    packed, names = call(
        pack_kernel,
        (far(blk, 6, h_dev, LANES), struct(NEIGH, blk, dtype=jnp.int32)),
        [ANY] * 4,
        1 << 20,
        [
            pltpu.VMEM((2, h_dev, nodes_dev), F32),
            pltpu.VMEM((h_dev, nodes_dev), F32),
            pltpu.VMEM((NEIGH, blk), jnp.int32),
            pltpu.VMEM((NEIGH, blk), jnp.int32),
            pltpu.SemaphoreType.DMA((4,)),
        ],
    )(krylov_basis, cond_time, neighbours.T, pattern.T)
    got = near(exchange(packed, HARM))
    pairs = [
        (g * harm + s, (g + offset) * harm + s)
        for s, offset in enumerate(OFFSETS)
        for g in range(groups)
        if 0 <= g + offset < groups
    ]
    named_by = lax.ppermute(near(names), NODE_HARM, pairs)
    high, low = spectral_tables()
    turned = call(
        turn_kernel,
        (
            struct(BS, BS),
            far(NEIGH, blk, dtype=jnp.int32),
            struct(*capacity.shape),
            struct(*high.shape, dtype=BF16),
            struct(*low.shape, dtype=BF16),
        ),
        [ANY] * 5,
        1 << 24,
        [
            pltpu.VMEM((BS, BS), F32),
            pltpu.SMEM((NEIGH, blk), jnp.int32),
            pltpu.SMEM((groups,), jnp.int32),
            pltpu.SemaphoreType.DMA((5,)),
        ],
        out_specs=(VMEM, SMEM, VMEM, VMEM, VMEM),
    )(names, diag_blocks, capacity, jnp.asarray(high), jnp.asarray(low))
    turned, where, *tables = turned
    solved, direct = call(
        solve_kernel,
        (struct(2 * H, BS), struct(2 * H, BS)),
        [VMEM] * 2,
        1 << 29,
        [pltpu.VMEM((3, 2, BS, BS), BF16)],
    )(got, near(turned))
    send_cols = call(column_kernel, far(harm, 9, h_dev, LANES), [VMEM] * 7, 1 << 27)(
        got, near(solved), near(direct), *map(near, tables), near(named_by)
    )
    back = near(exchange(send_cols, HARM))
    halves = call(
        halve_kernel,
        far(blk, NEIGH, 2, BS, BS, dtype=BF16),
        [ANY],
        1 << 24,
        [
            pltpu.VMEM(coupling.shape, F32),
            pltpu.VMEM((blk, NEIGH, 2, BS, BS), BF16),
            pltpu.SemaphoreType.DMA((blk,)),
            pltpu.SemaphoreType.DMA((blk,)),
        ],
        out_specs=ANY,
    )(coupling)
    send_named = call(
        select_kernel, struct(groups, 2, 4, h_dev, LANES), [VMEM], 1 << 34, limit=32 << 20
    )(back)
    named = exchange(near(send_named), NODE)
    gram = call(gram_kernel, far(1, LANES), [VMEM], 1 << 24, lanes)(krylov)
    image, send_sums = call(
        image_kernel,
        (struct(2, h_dev, nodes_dev), struct(world, LANES)),
        [VMEM] * 6,
        1 << 28,
        lanes,
        limit=32 << 20,
    )(near(where), near(named), near(halves), back, krylov, near(gram))
    sums = near(exchange(send_sums, NODE_HARM))
    count = world * h_dev * nodes_dev
    vector, proj, norm = call(
        lambda *refs: rest_kernel(count, *refs),
        (far(2, h_dev, nodes_dev), far(2, KRY), far(1, 1)),
        [VMEM] * 3,
        1 << 24,
        limit=48 << 20,
    )(sums, near(image), krylov)
    return vector, proj, norm.reshape(())


def solution(mesh):
    finer = Mesh(mesh.devices.reshape(4, 4, 4, 2), ("node_0", "node_1", "harm_0", "harm_1"))
    placed = (
        P(None, None, HARM, NODE),
        P(HARM, NODE),
        P(NODE),
        P(NODE, None, None),
        P(NODE, None, None, None),
        P(NODE, None),
        P(NODE, None),
    )

    return jax.shard_map(
        per_device,
        mesh=finer,
        in_specs=placed,
        out_specs=(P(None, HARM, NODE), P(), P()),
        check_vma=False,
    )
```

```python
import math

import jax
import jax.numpy as jnp
import numpy as np
from jax import lax
from jax.experimental import pallas as pl
from jax.experimental.pallas import tpu as pltpu
from jax.sharding import Mesh
from jax.sharding import PartitionSpec as P

BS = 256
H = 64
NEIGH = 2
KRY = 8
HARM = ("harm_0", "harm_1")
NODE = ("node_0", "node_1")
NODE_HARM = ("node_0", "node_1", "harm_0", "harm_1")
HARM_NODE = ("harm_0", "harm_1", "node_0", "node_1")
ACROSS = ("node_1", "node_0")
F32 = jnp.float32
BF16 = jnp.bfloat16
LANES = 128
CODE = 16
OFFSETS = (1, 2, 3, -1, -2, -3)
GRAM = 64
SMEM = pl.BlockSpec(memory_space=pltpu.SMEM)
VMEM = pl.BlockSpec(memory_space=pltpu.VMEM)
ANY = pl.BlockSpec(memory_space=pl.ANY)


def spectral_tables():
    steps = np.arange(H)
    angles = (steps[:, None] * steps[None, :] % H) * (2.0 * math.pi / H)
    cosine = np.cos(angles) / math.sqrt(H)
    sine = np.sin(angles) / math.sqrt(H)
    table = np.block([[cosine, -sine], [sine, cosine]]).astype(np.float32)
    both = np.stack([table, table.T])
    high = both.astype(jnp.bfloat16)
    low = (both - high.astype(np.float32)).astype(jnp.bfloat16)
    return high, low


def split(x):
    high = x.astype(BF16)
    return high, (x - high.astype(F32)).astype(BF16)


def mm(a, b):
    return jnp.dot(a, b, preferred_element_type=F32)


def rows_mm(x, w_high, w_low, product=mm):
    rows = x.shape[0]
    high, low = split(x)
    both = product(jnp.concatenate([high, low], axis=0), w_high)
    return both[:rows] + both[rows:] + product(high, w_low)


def in_turn(group):
    row = lax.div(group, lax.axis_size("node_1"))
    return (group - row * lax.axis_size("node_1")) * lax.axis_size("node_0") + row


def sublane_sum(x):
    return jnp.sum(x, axis=0, keepdims=True)


def rows_to_lanes(rows):
    return sublane_sum(jnp.transpose(rows))


def wide(ref, at, part):
    return jnp.concatenate([ref[at, 2 * part], ref[at, 2 * part + 1]], axis=1)


def pack_kernel(k_ref, cond_ref, nb_ref, pat_ref, out_ref, names_ref, v, cond, nb, pat, sems):
    copies = [
        pltpu.make_async_copy(source, target, sems.at[at])
        for at, (source, target) in enumerate(
            ((k_ref.at[KRY - 1], v), (cond_ref, cond), (nb_ref, nb), (pat_ref, pat))
        )
    ]
    for copy in copies:
        copy.start()
    for copy in copies:
        copy.wait()
    names_ref[...] = jnp.where(pat[...] > 0, nb[...], -1)
    for b in range(out_ref.shape[0]):
        for t in range(2):
            cols = slice(BS * b + LANES * t, BS * b + LANES * (t + 1))
            out_ref[b, t] = v[0, :, cols]
            out_ref[b, 2 + t] = v[1, :, cols]
            out_ref[b, 4 + t] = cond[:, cols]


def turn_kernel(
    names_ref, diag_ref, cap_ref, high_ref, low_ref, t_ref, where_ref, cap_out, high_out, low_out, held, names, least, sems
):
    copies = [
        pltpu.make_async_copy(source, target, sems.at[at])
        for at, (source, target) in enumerate(
            (
                (diag_ref.at[lax.axis_index(HARM)], held),
                (names_ref, names),
                (cap_ref, cap_out),
                (high_ref, high_out),
                (low_ref, low_out),
            )
        )
    ]
    for copy in copies:
        copy.start()
    copies[1].wait()
    blk = names.shape[1]
    for q in range(least.shape[0]):
        least[q] = blk
    for j in range(NEIGH):
        for b in range(blk):
            name = names[j, b]
            group = lax.div(name, blk)
            local = name - group * blk

            @pl.when(name >= 0)
            def _():
                least[group] = jnp.minimum(least[group], local)

    for j in range(NEIGH):
        for b in range(blk):
            name = names[j, b]
            group = lax.div(jnp.maximum(name, 0), blk)
            slot = jnp.where(name - group * blk == least[group], 0, 1)
            where_ref[j, b] = jnp.where(name >= 0, 2 * in_turn(group) + slot, -1)
    copies[0].wait()
    t_ref[...] = jnp.transpose(held[...])
    for copy in copies[2:]:
        copy.wait()


def gram_kernel(k_ref, gram_ref, rows):
    rows[...] = jnp.zeros_like(rows)
    chunks = k_ref.shape[3] // LANES
    for m in range(KRY):
        real = [None] * KRY
        imag = [None] * KRY
        for c in range(chunks):
            cols = slice(LANES * c, LANES * (c + 1))
            mr, mi = k_ref[m, 0, :, cols], k_ref[m, 1, :, cols]
            for n in range(m, KRY):
                nr, ni = (mr, mi) if n == m else (k_ref[n, 0, :, cols], k_ref[n, 1, :, cols])
                r = mr * nr + mi * ni
                real[n] = r if c == 0 else real[n] + r
                if n > m:
                    i = mr * ni - mi * nr
                    imag[n] = i if c == 0 else imag[n] + i
        for n in range(m, KRY):
            at = GRAM + KRY * m + n
            rows[at : at + 1] = sublane_sum(real[n])
            if n > m:
                at = GRAM + KRY * n + m
                rows[at : at + 1] = sublane_sum(imag[n])
    gram_ref[...] = rows_to_lanes(rows[...])


def named_code(names, blk):
    group = lax.div(names, blk)
    local = (names - group * blk).astype(F32)
    hit = (group == lax.axis_index(NODE)) & (names >= 0)

    def over_all(x, reduce):
        return reduce(reduce(x, axis=1, keepdims=True), axis=0, keepdims=True)

    least = over_all(jnp.where(hit, local, blk - 1.0), jnp.min)
    greatest = over_all(jnp.where(hit, local, 0.0), jnp.max)
    return jnp.broadcast_to(least * CODE + greatest, (8, LANES))


def solve_kernel(got_ref, t_ref, u_ref, direct_ref, e_ref):
    sources = got_ref.shape[0]
    powers = e_ref.shape[0]
    mean = sublane_sum(conductance(got_ref)) * (1.0 / H)
    d = 1.0 / mean
    u = jnp.concatenate([wide(got_ref, s, p) for p in range(2) for s in range(sources)], axis=0) * d
    power = t_ref[...] * (-d)
    for p in range(powers):
        e_ref[p, 0], e_ref[p, 1] = split(power)
        high, low = e_ref[p, 0], e_ref[p, 1]
        u = u + rows_mm(u, high, low)
        if p < powers - 1:
            power = mm(high, high) + mm(low, high) + mm(high, low)
    high, low = e_ref[powers - 1, 0], e_ref[powers - 1, 1]
    u = u + rows_mm(rows_mm(u, high, low), high, low)
    u_ref[...] = u
    direct_ref[...] = rows_mm(u, e_ref[0, 0], e_ref[0, 1]) * (-mean)


def conductance(got_ref):
    return jnp.concatenate([wide(got_ref, s, 2) for s in range(got_ref.shape[0])], axis=0)


def column_kernel(got_ref, u_ref, direct_ref, cap_ref, high_ref, low_ref, names_ref, out_ref):
    own = lax.axis_index(HARM)
    sources = got_ref.shape[0]
    u = u_ref[...]
    cond = conductance(got_ref)

    def transform(way, x):
        high, low = split(x)
        table = high_ref[way]
        return mm(table, high) + mm(table, low) + mm(low_ref[way], high)

    driven = transform(0, u) * jnp.concatenate([cond, cond], axis=0)
    image = direct_ref[...] + transform(1, driven)
    cap = cap_ref[pl.ds(pl.multiple_of(own * BS, BS), BS)].reshape(1, BS)
    harmonic = lax.broadcasted_iota(jnp.int32, (H, BS), 0)
    omega = jnp.where(harmonic < H // 2, harmonic, harmonic - H)
    react = omega.astype(F32) * cap
    real = image[:H] - react * u[H:]
    imag = image[H:] + react * u[:H]
    step = H // sources
    code = named_code(names_ref[...], sources)
    for s in range(sources):
        rows = slice(step * s, step * (s + 1))
        later = slice(H + step * s, H + step * (s + 1))
        for at, part in enumerate((real[rows], imag[rows], u[rows], u[later])):
            out_ref[s, 2 * at] = part[:, :LANES]
            out_ref[s, 2 * at + 1] = part[:, LANES:]
        out_ref[s, 8] = code


def select_kernel(back_ref, send_ref):
    me = lax.axis_index(NODE)
    groups = send_ref.shape[0]
    for at, offset in enumerate(OFFSETS):
        group = me - offset

        @pl.when((group >= 0) & (group < groups))
        def _():
            code = back_ref[at, 8, 0:1, 0:1][0, 0].astype(jnp.int32)
            least = lax.div(code, CODE)
            for slot, b in enumerate((least, code - least * CODE)):
                send_ref[in_turn(group), slot] = back_ref[b, 4:8]


def halve_kernel(c_ref, out_ref, held, halves, in_sems, out_sems):
    blk = held.shape[0]
    reads = [pltpu.make_async_copy(c_ref.at[b], held.at[b], in_sems.at[b]) for b in range(blk)]
    writes = [pltpu.make_async_copy(halves.at[b], out_ref.at[b], out_sems.at[b]) for b in range(blk)]
    for read in reads:
        read.start()
    for b in range(blk):
        reads[b].wait()
        for j in range(NEIGH):
            halves[b, j, 0], halves[b, j, 1] = split(jnp.transpose(held[b, j]))
        writes[b].start()
    for write in writes:
        write.wait()


def image_kernel(where_ref, got_ref, halves_ref, back_ref, k_ref, gram_ref, image_ref, send_ref, rows):
    blk = halves_ref.shape[0]
    half = image_ref.shape[1]
    for b in range(blk):
        total = jnp.concatenate([wide(back_ref, b, 0), wide(back_ref, b, 1)], axis=0)
        for j in range(NEIGH):
            at = where_ref[j : j + 1, b : b + 1][0, 0]
            group = lax.div(jnp.maximum(at, 0), 2)
            x = got_ref[group, jnp.maximum(at - 2 * group, 0)]
            x = jnp.concatenate([jnp.concatenate([x[2 * p], x[2 * p + 1]], axis=1) for p in range(2)], axis=0)
            x = jnp.where(at >= 0, x, 0.0)
            total = total + rows_mm(x, halves_ref[b, j, 0], halves_ref[b, j, 1])
        cols = slice(b * BS, (b + 1) * BS)
        image_ref[0, :, cols] = total[:half]
        image_ref[1, :, cols] = total[half:]

    chunks = k_ref.shape[3] // LANES
    real = [None] * KRY
    imag = [None] * KRY
    squares = None
    for c in range(chunks):
        cols = slice(LANES * c, LANES * (c + 1))
        ir, ii = image_ref[0, :, cols], image_ref[1, :, cols]
        both = ir * ir + ii * ii
        squares = both if c == 0 else squares + both
        for m in range(KRY):
            mr, mi = k_ref[m, 0, :, cols], k_ref[m, 1, :, cols]
            r = mr * ir + mi * ii
            i = mr * ii - mi * ir
            real[m] = r if c == 0 else real[m] + r
            imag[m] = i if c == 0 else imag[m] + i
    rows[...] = jnp.zeros_like(rows)
    for m in range(KRY):
        rows[m : m + 1] = sublane_sum(real[m])
        rows[KRY + m : KRY + m + 1] = sublane_sum(imag[m])
    rows[2 * KRY : 2 * KRY + 1] = sublane_sum(squares)
    row = rows_to_lanes(rows[...]) + gram_ref[...]
    send_ref[...] = jnp.broadcast_to(row, send_ref.shape)


def rest_kernel(count, got_ref, image_ref, k_ref, vector_ref, proj_ref, norm_ref):
    totals = sublane_sum(got_ref[...]) * (1.0 / count)
    lane = lax.broadcasted_iota(jnp.int32, totals.shape, 1)

    def at(q):
        return jnp.broadcast_to(totals[:, q : q + 1], totals.shape)

    pr = [at(m) for m in range(KRY)]
    pi = [at(KRY + m) for m in range(KRY)]
    row_r = row_i = col_r = col_i = jnp.zeros_like(totals)
    row_of = (lane - GRAM) // KRY
    col_of = (lane - GRAM) - row_of * KRY
    for m in range(KRY):
        row_r = jnp.where(row_of == m, pr[m], row_r)
        row_i = jnp.where(row_of == m, pi[m], row_i)
        col_r = jnp.where(col_of == m, pr[m], col_r)
        col_i = jnp.where(col_of == m, pi[m], col_i)
    upper = row_r * col_r + row_i * col_i
    lower = col_i * row_r - col_r * row_i
    weight = jnp.where(row_of == col_of, upper, 2.0 * jnp.where(row_of < col_of, upper, lower))
    weight = jnp.where(lane >= GRAM, weight, 0.0)
    weight = jnp.where(lane < 2 * KRY, -2.0 * totals, weight)
    weight = jnp.where(lane == 2 * KRY, 1.0, weight)
    squares = jnp.sum(totals * weight, axis=1, keepdims=True)
    norm = jnp.sqrt(squares + 1e-06)
    norm_ref[...] = norm
    for m in range(KRY):
        proj_ref[0:1, m : m + 1] = pr[m][:, 0:1]
        proj_ref[1:2, m : m + 1] = pi[m][:, 0:1]
    half = k_ref.shape[2]
    scale = jnp.broadcast_to(1.0 / norm, (half, LANES))
    pr = [jnp.broadcast_to(x, (half, LANES)) for x in pr]
    pi = [jnp.broadcast_to(x, (half, LANES)) for x in pi]
    for c in range(k_ref.shape[3] // LANES):
        cols = slice(LANES * c, LANES * (c + 1))
        real, imag = image_ref[0, :, cols], image_ref[1, :, cols]
        for m in range(KRY):
            mr, mi = k_ref[m, 0, :, cols], k_ref[m, 1, :, cols]
            real = real - (pr[m] * mr - pi[m] * mi)
            imag = imag - (pr[m] * mi + pi[m] * mr)
        vector_ref[0, :, cols] = real * scale
        vector_ref[1, :, cols] = imag * scale


def struct(*dims, dtype=F32):
    return pltpu.VMEM(dims, dtype)


def far(*dims, dtype=F32):
    return jax.ShapeDtypeStruct(dims, dtype)


def near(x):
    return pltpu.with_memory_space_constraint(x, pltpu.VMEM)


def call(kernel, out_shape, in_specs, flops, scratch=(), out_specs=None, limit=60 * 1024 * 1024, aliases=None):
    single = not isinstance(out_shape, tuple)
    return pl.pallas_call(
        kernel,
        out_shape=out_shape,
        in_specs=in_specs,
        out_specs=out_specs or (VMEM if single else (VMEM,) * len(out_shape)),
        scratch_shapes=list(scratch),
        cost_estimate=pl.CostEstimate(flops=flops, bytes_accessed=1 << 20, transcendentals=0),
        compiler_params=pltpu.CompilerParams(vmem_limit_bytes=limit),
        input_output_aliases=aliases or {},
    )


def exchange(x, axes):
    return lax.all_to_all(x, axes, split_axis=0, concat_axis=0, tiled=True)


def per_device(krylov_basis, cond_time, capacity, diag_blocks, coupling, neighbours, pattern):
    h_dev = krylov_basis.shape[2]
    nodes_dev = krylov_basis.shape[3]
    blk = diag_blocks.shape[0]
    harm = lax.axis_size(HARM)
    groups = lax.axis_size(NODE)
    world = groups * harm
    lanes = [pltpu.VMEM((LANES, LANES), F32)]
    krylov = near(krylov_basis)

    packed, names = call(
        pack_kernel,
        (far(blk, 6, h_dev, LANES), struct(NEIGH, blk, dtype=jnp.int32)),
        [ANY] * 4,
        1 << 20,
        [
            pltpu.VMEM((2, h_dev, nodes_dev), F32),
            pltpu.VMEM((h_dev, nodes_dev), F32),
            pltpu.VMEM((NEIGH, blk), jnp.int32),
            pltpu.VMEM((NEIGH, blk), jnp.int32),
            pltpu.SemaphoreType.DMA((4,)),
        ],
    )(krylov_basis, cond_time, neighbours.T, pattern.T)
    got = near(exchange(packed, HARM))
    pairs = [
        (g * harm + s, (g + offset) * harm + s)
        for s, offset in enumerate(OFFSETS)
        for g in range(groups)
        if 0 <= g + offset < groups
    ]
    named_by = lax.ppermute(near(names), NODE_HARM, pairs)
    high, low = spectral_tables()
    turned = call(
        turn_kernel,
        (
            struct(BS, BS),
            far(NEIGH, blk, dtype=jnp.int32),
            struct(*capacity.shape),
            struct(*high.shape, dtype=BF16),
            struct(*low.shape, dtype=BF16),
        ),
        [ANY] * 5,
        1 << 24,
        [
            pltpu.VMEM((BS, BS), F32),
            pltpu.SMEM((NEIGH, blk), jnp.int32),
            pltpu.SMEM((groups,), jnp.int32),
            pltpu.SemaphoreType.DMA((5,)),
        ],
        out_specs=(VMEM, SMEM, VMEM, VMEM, VMEM),
    )(names, diag_blocks, capacity, jnp.asarray(high), jnp.asarray(low))
    turned, where, *tables = turned
    solved, direct = call(
        solve_kernel,
        (struct(2 * H, BS), struct(2 * H, BS)),
        [VMEM] * 2,
        1 << 29,
        [pltpu.VMEM((3, 2, BS, BS), BF16)],
    )(got, near(turned))
    send_cols = call(column_kernel, far(harm, 9, h_dev, LANES), [VMEM] * 7, 1 << 27)(
        got, near(solved), near(direct), *map(near, tables), near(named_by)
    )
    back = near(exchange(send_cols, HARM))
    halves = call(
        halve_kernel,
        far(blk, NEIGH, 2, BS, BS, dtype=BF16),
        [ANY],
        1 << 24,
        [
            pltpu.VMEM(coupling.shape, F32),
            pltpu.VMEM((blk, NEIGH, 2, BS, BS), BF16),
            pltpu.SemaphoreType.DMA((blk,)),
            pltpu.SemaphoreType.DMA((blk,)),
        ],
        out_specs=ANY,
    )(coupling)
    send_named = call(
        select_kernel, struct(groups, 2, 4, h_dev, LANES), [VMEM], 1 << 34, limit=32 << 20
    )(back)
    named = exchange(near(send_named), ACROSS)
    gram = call(gram_kernel, far(1, LANES), [VMEM], 1 << 24, lanes)(krylov)
    image, send_sums = call(
        image_kernel,
        (struct(2, h_dev, nodes_dev), struct(world, LANES)),
        [VMEM] * 6,
        1 << 28,
        lanes,
        limit=32 << 20,
    )(near(where), near(named), near(halves), back, krylov, near(gram))
    sums = near(exchange(send_sums, HARM_NODE))
    count = world * h_dev * nodes_dev
    vector, proj, norm = call(
        lambda *refs: rest_kernel(count, *refs),
        (far(2, h_dev, nodes_dev), far(2, KRY), far(1, 1)),
        [VMEM] * 3,
        1 << 24,
        limit=48 << 20,
    )(sums, near(image), krylov)
    return vector, proj, norm.reshape(())


def solution(mesh):
    finer = Mesh(mesh.devices.reshape(4, 4, 4, 2), ("node_0", "node_1", "harm_0", "harm_1"))
    placed = (
        P(None, None, HARM, NODE),
        P(HARM, NODE),
        P(NODE),
        P(NODE, None, None),
        P(NODE, None, None, None),
        P(NODE, None),
        P(NODE, None),
    )

    return jax.shard_map(
        per_device,
        mesh=finer,
        in_specs=placed,
        out_specs=(P(None, HARM, NODE), P(), P()),
        check_vma=False,
    )
```

```python
import math

import jax
import jax.numpy as jnp
import numpy as np
from jax import lax
from jax.experimental import pallas as pl
from jax.experimental.pallas import tpu as pltpu
from jax.sharding import Mesh
from jax.sharding import PartitionSpec as P

BS = 256
H = 64
NEIGH = 2
KRY = 8
HARM = ("harm_0", "harm_1")
NODE = ("node_0", "node_1")
NODE_HARM = ("node_0", "node_1", "harm_0", "harm_1")
F32 = jnp.float32
BF16 = jnp.bfloat16
LANES = 128
CODE = 16
OFFSETS = (1, 2, 3, -1, -2, -3)
GRAM = 64
SMEM = pl.BlockSpec(memory_space=pltpu.SMEM)
VMEM = pl.BlockSpec(memory_space=pltpu.VMEM)
ANY = pl.BlockSpec(memory_space=pl.ANY)


def spectral_tables():
    steps = np.arange(H)
    angles = (steps[:, None] * steps[None, :] % H) * (2.0 * math.pi / H)
    cosine = np.cos(angles) / math.sqrt(H)
    sine = np.sin(angles) / math.sqrt(H)
    table = np.block([[cosine, -sine], [sine, cosine]]).astype(np.float32)
    both = np.stack([table, table.T])
    high = both.astype(jnp.bfloat16)
    low = (both - high.astype(np.float32)).astype(jnp.bfloat16)
    return high, low


def split(x):
    high = x.astype(BF16)
    return high, (x - high.astype(F32)).astype(BF16)


def mm(a, b):
    return jnp.dot(a, b, preferred_element_type=F32)


def rows_mm(x, w_high, w_low, product=mm):
    rows = x.shape[0]
    high, low = split(x)
    both = product(jnp.concatenate([high, low], axis=0), w_high)
    return both[:rows] + both[rows:] + product(high, w_low)


def sublane_sum(x):
    return jnp.sum(x, axis=0, keepdims=True)


def rows_to_lanes(rows):
    return sublane_sum(jnp.transpose(rows))


def wide(ref, at, part):
    return jnp.concatenate([ref[at, 2 * part], ref[at, 2 * part + 1]], axis=1)


def pack_kernel(k_ref, cond_ref, nb_ref, pat_ref, out_ref, names_ref, v, cond, nb, pat, sems):
    copies = [
        pltpu.make_async_copy(source, target, sems.at[at])
        for at, (source, target) in enumerate(
            ((k_ref.at[KRY - 1], v), (cond_ref, cond), (nb_ref, nb), (pat_ref, pat))
        )
    ]
    for copy in copies:
        copy.start()
    for copy in copies:
        copy.wait()
    names_ref[...] = jnp.where(pat[...] > 0, nb[...], -1)
    for b in range(out_ref.shape[0]):
        for t in range(2):
            cols = slice(BS * b + LANES * t, BS * b + LANES * (t + 1))
            out_ref[b, t] = v[0, :, cols]
            out_ref[b, 2 + t] = v[1, :, cols]
            out_ref[b, 4 + t] = cond[:, cols]


def turn_kernel(
    names_ref, diag_ref, cap_ref, high_ref, low_ref, t_ref, where_ref, cap_out, high_out, low_out, held, names, least, sems
):
    copies = [
        pltpu.make_async_copy(source, target, sems.at[at])
        for at, (source, target) in enumerate(
            (
                (diag_ref.at[lax.axis_index(HARM)], held),
                (names_ref, names),
                (cap_ref, cap_out),
                (high_ref, high_out),
                (low_ref, low_out),
            )
        )
    ]
    for copy in copies:
        copy.start()
    copies[1].wait()
    blk = names.shape[1]
    for q in range(least.shape[0]):
        least[q] = blk
    for j in range(NEIGH):
        for b in range(blk):
            name = names[j, b]
            group = lax.div(name, blk)
            local = name - group * blk

            @pl.when(name >= 0)
            def _():
                least[group] = jnp.minimum(least[group], local)

    for j in range(NEIGH):
        for b in range(blk):
            name = names[j, b]
            group = lax.div(jnp.maximum(name, 0), blk)
            slot = jnp.where(name - group * blk == least[group], 0, 1)
            where_ref[j, b] = jnp.where(name >= 0, 2 * group + slot, -1)
    copies[0].wait()
    t_ref[...] = jnp.transpose(held[...])
    for copy in copies[2:]:
        copy.wait()


def gram_kernel(k_ref, gram_ref, rows):
    rows[...] = jnp.zeros_like(rows)
    chunks = k_ref.shape[3] // LANES
    for m in range(KRY):
        real = [None] * KRY
        imag = [None] * KRY
        for c in range(chunks):
            cols = slice(LANES * c, LANES * (c + 1))
            mr, mi = k_ref[m, 0, :, cols], k_ref[m, 1, :, cols]
            for n in range(m, KRY):
                nr, ni = (mr, mi) if n == m else (k_ref[n, 0, :, cols], k_ref[n, 1, :, cols])
                r = mr * nr + mi * ni
                real[n] = r if c == 0 else real[n] + r
                if n > m:
                    i = mr * ni - mi * nr
                    imag[n] = i if c == 0 else imag[n] + i
        for n in range(m, KRY):
            at = GRAM + KRY * m + n
            rows[at : at + 1] = sublane_sum(real[n])
            if n > m:
                at = GRAM + KRY * n + m
                rows[at : at + 1] = sublane_sum(imag[n])
    gram_ref[...] = rows_to_lanes(rows[...])


def named_code(names, blk):
    group = lax.div(names, blk)
    local = (names - group * blk).astype(F32)
    hit = (group == lax.axis_index(NODE)) & (names >= 0)

    def over_all(x, reduce):
        return reduce(reduce(x, axis=1, keepdims=True), axis=0, keepdims=True)

    least = over_all(jnp.where(hit, local, blk - 1.0), jnp.min)
    greatest = over_all(jnp.where(hit, local, 0.0), jnp.max)
    return jnp.broadcast_to(least * CODE + greatest, (8, LANES))


def solve_kernel(got_ref, t_ref, cap_ref, high_ref, low_ref, u_ref, image_ref, e_ref):
    own = lax.axis_index(HARM)
    sources = got_ref.shape[0]
    powers = e_ref.shape[0]
    cond = jnp.concatenate([wide(got_ref, s, 2) for s in range(sources)], axis=0)
    mean = sublane_sum(cond) * (1.0 / H)
    d = 1.0 / mean
    u = jnp.concatenate([wide(got_ref, s, p) for p in range(2) for s in range(sources)], axis=0) * d
    power = t_ref[...] * (-d)
    for p in range(powers):
        e_ref[p, 0], e_ref[p, 1] = split(power)
        high, low = e_ref[p, 0], e_ref[p, 1]
        u = u + rows_mm(u, high, low)
        if p < powers - 1:
            power = mm(high, high) + mm(low, high) + mm(high, low)
    u_ref[...] = u
    direct = rows_mm(u, e_ref[0, 0], e_ref[0, 1]) * (-mean)

    def transform(way, x):
        high, low = split(x)
        table = high_ref[way]
        return mm(table, high) + mm(table, low) + mm(low_ref[way], high)

    driven = transform(0, u) * jnp.concatenate([cond, cond], axis=0)
    image = direct + transform(1, driven)
    cap = cap_ref[pl.ds(pl.multiple_of(own * BS, BS), BS)].reshape(1, BS)
    harmonic = lax.broadcasted_iota(jnp.int32, (H, BS), 0)
    omega = jnp.where(harmonic < H // 2, harmonic, harmonic - H)
    react = omega.astype(F32) * cap
    image_ref[:H] = image[:H] - react * u[H:]
    image_ref[H:] = image[H:] + react * u[:H]


def column_kernel(u_ref, image_ref, names_ref, out_ref):
    sources = out_ref.shape[0]
    step = H // sources
    code = named_code(names_ref[...], sources)
    for s in range(sources):
        for p in range(2):
            rows = slice(H * p + step * s, H * p + step * (s + 1))
            for t in range(2):
                cols = slice(LANES * t, LANES * (t + 1))
                out_ref[s, 2 * p + t] = image_ref[rows, cols]
                out_ref[s, 4 + 2 * p + t] = u_ref[rows, cols]
        out_ref[s, 8] = code


def select_kernel(back_ref, send_ref):
    me = lax.axis_index(NODE)
    groups = send_ref.shape[0]
    for at, offset in enumerate(OFFSETS):
        group = me - offset

        @pl.when((group >= 0) & (group < groups))
        def _():
            code = back_ref[at, 8, 0:1, 0:1][0, 0].astype(jnp.int32)
            least = lax.div(code, CODE)
            for slot, b in enumerate((least, code - least * CODE)):
                send_ref[group, slot] = back_ref[b, 4:8]


def halve_kernel(c_ref, out_ref, held, halves, in_sems, out_sems):
    blk = held.shape[0]
    reads = [pltpu.make_async_copy(c_ref.at[b], held.at[b], in_sems.at[b]) for b in range(blk)]
    writes = [pltpu.make_async_copy(halves.at[b], out_ref.at[b], out_sems.at[b]) for b in range(blk)]
    for read in reads:
        read.start()
    for b in range(blk):
        reads[b].wait()
        for j in range(NEIGH):
            halves[b, j, 0], halves[b, j, 1] = split(jnp.transpose(held[b, j]))
        writes[b].start()
    for write in writes:
        write.wait()


def image_kernel(where_ref, got_ref, halves_ref, back_ref, k_ref, gram_ref, image_ref, send_ref, rows):
    blk = halves_ref.shape[0]
    half = image_ref.shape[1]
    for b in range(blk):
        total = jnp.concatenate([wide(back_ref, b, 0), wide(back_ref, b, 1)], axis=0)
        for j in range(NEIGH):
            at = where_ref[j : j + 1, b : b + 1][0, 0]
            group = lax.div(jnp.maximum(at, 0), 2)
            x = got_ref[group, jnp.maximum(at - 2 * group, 0)]
            x = jnp.concatenate([jnp.concatenate([x[2 * p], x[2 * p + 1]], axis=1) for p in range(2)], axis=0)
            x = jnp.where(at >= 0, x, 0.0)
            total = total + rows_mm(x, halves_ref[b, j, 0], halves_ref[b, j, 1])
        cols = slice(b * BS, (b + 1) * BS)
        image_ref[0, :, cols] = total[:half]
        image_ref[1, :, cols] = total[half:]

    chunks = k_ref.shape[3] // LANES
    real = [None] * KRY
    imag = [None] * KRY
    squares = None
    for c in range(chunks):
        cols = slice(LANES * c, LANES * (c + 1))
        ir, ii = image_ref[0, :, cols], image_ref[1, :, cols]
        both = ir * ir + ii * ii
        squares = both if c == 0 else squares + both
        for m in range(KRY):
            mr, mi = k_ref[m, 0, :, cols], k_ref[m, 1, :, cols]
            r = mr * ir + mi * ii
            i = mr * ii - mi * ir
            real[m] = r if c == 0 else real[m] + r
            imag[m] = i if c == 0 else imag[m] + i
    rows[...] = jnp.zeros_like(rows)
    for m in range(KRY):
        rows[m : m + 1] = sublane_sum(real[m])
        rows[KRY + m : KRY + m + 1] = sublane_sum(imag[m])
    rows[2 * KRY : 2 * KRY + 1] = sublane_sum(squares)
    row = rows_to_lanes(rows[...]) + gram_ref[...]
    send_ref[...] = jnp.broadcast_to(row, send_ref.shape)


def rest_kernel(count, got_ref, image_ref, k_ref, vector_ref, proj_ref, norm_ref):
    totals = sublane_sum(got_ref[...]) * (1.0 / count)
    lane = lax.broadcasted_iota(jnp.int32, totals.shape, 1)

    def at(q):
        return jnp.broadcast_to(totals[:, q : q + 1], totals.shape)

    pr = [at(m) for m in range(KRY)]
    pi = [at(KRY + m) for m in range(KRY)]
    row_r = row_i = col_r = col_i = jnp.zeros_like(totals)
    row_of = (lane - GRAM) // KRY
    col_of = (lane - GRAM) - row_of * KRY
    for m in range(KRY):
        row_r = jnp.where(row_of == m, pr[m], row_r)
        row_i = jnp.where(row_of == m, pi[m], row_i)
        col_r = jnp.where(col_of == m, pr[m], col_r)
        col_i = jnp.where(col_of == m, pi[m], col_i)
    upper = row_r * col_r + row_i * col_i
    lower = col_i * row_r - col_r * row_i
    weight = jnp.where(row_of == col_of, upper, 2.0 * jnp.where(row_of < col_of, upper, lower))
    weight = jnp.where(lane >= GRAM, weight, 0.0)
    weight = jnp.where(lane < 2 * KRY, -2.0 * totals, weight)
    weight = jnp.where(lane == 2 * KRY, 1.0, weight)
    squares = jnp.sum(totals * weight, axis=1, keepdims=True)
    norm = jnp.sqrt(squares + 1e-06)
    norm_ref[...] = norm
    for m in range(KRY):
        proj_ref[0:1, m : m + 1] = pr[m][:, 0:1]
        proj_ref[1:2, m : m + 1] = pi[m][:, 0:1]
    half = k_ref.shape[2]
    scale = jnp.broadcast_to(1.0 / norm, (half, LANES))
    pr = [jnp.broadcast_to(x, (half, LANES)) for x in pr]
    pi = [jnp.broadcast_to(x, (half, LANES)) for x in pi]
    for c in range(k_ref.shape[3] // LANES):
        cols = slice(LANES * c, LANES * (c + 1))
        real, imag = image_ref[0, :, cols], image_ref[1, :, cols]
        for m in range(KRY):
            mr, mi = k_ref[m, 0, :, cols], k_ref[m, 1, :, cols]
            real = real - (pr[m] * mr - pi[m] * mi)
            imag = imag - (pr[m] * mi + pi[m] * mr)
        vector_ref[0, :, cols] = real * scale
        vector_ref[1, :, cols] = imag * scale


def struct(*dims, dtype=F32):
    return pltpu.VMEM(dims, dtype)


def far(*dims, dtype=F32):
    return jax.ShapeDtypeStruct(dims, dtype)


def near(x):
    return pltpu.with_memory_space_constraint(x, pltpu.VMEM)


def call(kernel, out_shape, in_specs, flops, scratch=(), out_specs=None, limit=60 * 1024 * 1024, aliases=None):
    single = not isinstance(out_shape, tuple)
    return pl.pallas_call(
        kernel,
        out_shape=out_shape,
        in_specs=in_specs,
        out_specs=out_specs or (VMEM if single else (VMEM,) * len(out_shape)),
        scratch_shapes=list(scratch),
        cost_estimate=pl.CostEstimate(flops=flops, bytes_accessed=1 << 20, transcendentals=0),
        compiler_params=pltpu.CompilerParams(vmem_limit_bytes=limit),
        input_output_aliases=aliases or {},
    )


def exchange(x, axes):
    return lax.all_to_all(x, axes, split_axis=0, concat_axis=0, tiled=True)


def per_device(krylov_basis, cond_time, capacity, diag_blocks, coupling, neighbours, pattern):
    h_dev = krylov_basis.shape[2]
    nodes_dev = krylov_basis.shape[3]
    blk = diag_blocks.shape[0]
    harm = lax.axis_size(HARM)
    groups = lax.axis_size(NODE)
    world = groups * harm
    lanes = [pltpu.VMEM((LANES, LANES), F32)]
    krylov = near(krylov_basis)

    packed, names = call(
        pack_kernel,
        (far(blk, 6, h_dev, LANES), struct(NEIGH, blk, dtype=jnp.int32)),
        [ANY] * 4,
        1 << 20,
        [
            pltpu.VMEM((2, h_dev, nodes_dev), F32),
            pltpu.VMEM((h_dev, nodes_dev), F32),
            pltpu.VMEM((NEIGH, blk), jnp.int32),
            pltpu.VMEM((NEIGH, blk), jnp.int32),
            pltpu.SemaphoreType.DMA((4,)),
        ],
    )(krylov_basis, cond_time, neighbours.T, pattern.T)
    got = near(exchange(packed, HARM))
    pairs = [
        (g * harm + s, (g + offset) * harm + s)
        for s, offset in enumerate(OFFSETS)
        for g in range(groups)
        if 0 <= g + offset < groups
    ]
    named_by = lax.ppermute(near(names), NODE_HARM, pairs)
    high, low = spectral_tables()
    turned = call(
        turn_kernel,
        (
            struct(BS, BS),
            far(NEIGH, blk, dtype=jnp.int32),
            struct(*capacity.shape),
            struct(*high.shape, dtype=BF16),
            struct(*low.shape, dtype=BF16),
        ),
        [ANY] * 5,
        1 << 24,
        [
            pltpu.VMEM((BS, BS), F32),
            pltpu.SMEM((NEIGH, blk), jnp.int32),
            pltpu.SMEM((groups,), jnp.int32),
            pltpu.SemaphoreType.DMA((5,)),
        ],
        out_specs=(VMEM, SMEM, VMEM, VMEM, VMEM),
    )(names, diag_blocks, capacity, jnp.asarray(high), jnp.asarray(low))
    turned, where, *tables = turned
    solved, part = call(
        solve_kernel,
        (struct(2 * H, BS), struct(2 * H, BS)),
        [VMEM] * 5,
        1 << 29,
        [pltpu.VMEM((4, 2, BS, BS), BF16)],
    )(got, near(turned), *map(near, tables))
    send_cols = call(column_kernel, far(harm, 9, h_dev, LANES), [VMEM] * 3, 1 << 20)(
        near(solved), near(part), near(named_by)
    )
    back = near(exchange(send_cols, HARM))
    halves = call(
        halve_kernel,
        far(blk, NEIGH, 2, BS, BS, dtype=BF16),
        [ANY],
        1 << 24,
        [
            pltpu.VMEM(coupling.shape, F32),
            pltpu.VMEM((blk, NEIGH, 2, BS, BS), BF16),
            pltpu.SemaphoreType.DMA((blk,)),
            pltpu.SemaphoreType.DMA((blk,)),
        ],
        out_specs=ANY,
    )(coupling)
    send_named = call(
        select_kernel, struct(groups, 2, 4, h_dev, LANES), [VMEM], 1 << 34, limit=32 << 20
    )(back)
    named = exchange(near(send_named), NODE)
    gram = call(gram_kernel, far(1, LANES), [VMEM], 1 << 24, lanes)(krylov)
    image, send_sums = call(
        image_kernel,
        (struct(2, h_dev, nodes_dev), struct(world, LANES)),
        [VMEM] * 6,
        1 << 28,
        lanes,
        limit=32 << 20,
    )(near(where), near(named), near(halves), back, krylov, near(gram))
    sums = near(exchange(send_sums, NODE_HARM))
    count = world * h_dev * nodes_dev
    vector, proj, norm = call(
        lambda *refs: rest_kernel(count, *refs),
        (far(2, h_dev, nodes_dev), far(2, KRY), far(1, 1)),
        [VMEM] * 3,
        1 << 24,
        limit=48 << 20,
    )(sums, near(image), krylov)
    return vector, proj, norm.reshape(())


def solution(mesh):
    finer = Mesh(mesh.devices.reshape(4, 4, 4, 2), ("node_0", "node_1", "harm_0", "harm_1"))
    placed = (
        P(None, None, HARM, NODE),
        P(HARM, NODE),
        P(NODE),
        P(NODE, None, None),
        P(NODE, None, None, None),
        P(NODE, None),
        P(NODE, None),
    )

    return jax.shard_map(
        per_device,
        mesh=finer,
        in_specs=placed,
        out_specs=(P(None, HARM, NODE), P(), P()),
        check_vma=False,
    )
```
